512 devices in a mesh: tm: 128 (over y, z, core), group: 4 (over x).
Axes of the slice: x: 4, y: 8, z: 8, core: 2. Of those that a mesh axis runs over, the one named last changes fastest.
Arguments:
- values: float32 [1048576, 64], P(('tm', 'group')), may hold values from -6 to 6
- group_ids: int32 [1048576], P(('tm', 'group')), may hold values from 0 to 2047, as said below
- slot_of: int32 [2048], replicated, may hold values from 0 to 2047, each once
Outputs:
- running_mean: float32 [1048576, 64], P(('tm', 'group'))
- running_count: int32 [1048576], P(('tm', 'group'))
- closing_mean: float32 [2048, 64], P('group')
The draws below stay inside these ranges and needn't reach their ends.
Inputs may be any that keep to these rules, and one draw needn't show every extreme that they name: `slot_of`: a permutation of the slots; slot s belongs to index s // (2048 / 4) of the group axis. `group_ids`: some store groups may have no rows in the window.
All inputs are finite; a program needn't handle non-finite values.
Results may differ from the reference program's by a relative error of at most 0.0003.
Values sent between devices are 32-bit elements; how exact they have to be, the bound alone decides.
No kernel may reach another device: no remote copies, remote signals or barrier semaphores. Data moves between devices by JAX's collectives and lax.ppermute only.
A program may use at most 64 MiB of HBM per device.

```python
import math
import jax
import jax.numpy as jnp
from jax import lax

M = 64
G = 2048
ROWS = 1048576


def draw_group_ids(key, part):
    used = G - G // 16
    order_key = jax.random.fold_in(key, 11)
    reach_key = jax.random.fold_in(key, 23)
    rank_key = jax.random.fold_in(key, 37)
    order = jax.random.permutation(order_key, G)
    reach = jax.random.randint(reach_key, (ROWS,), 1, used + 1)
    rank = jax.random.randint(rank_key, (ROWS,), 0, reach)
    return jnp.take(order, rank).astype(jnp.int32)


def block_scale(key, extent, cuts, low, largest):
    def one(dim, parts):
        draws = jax.random.uniform(jax.random.fold_in(jax.random.fold_in(key, 6), dim), (parts,), jnp.float32, low / len(cuts), largest / len(cuts))
        return jnp.repeat(jnp.exp(draws), extent[dim] // parts).reshape((-1,) + (1,) * (len(extent) - dim - 1))

    loudness = one(*cuts[0])
    for cut in cuts[1:]:
        loudness = loudness * one(*cut)
    return loudness


def bell_draw(own_key, shape, scale, most, cuts=(), kind=jnp.bfloat16):
    level = block_scale(own_key, shape, cuts, -0.22, 0.18) if cuts else 1.0
    values = jax.random.normal(own_key, shape, jnp.float32) * scale * level
    return jnp.minimum(jnp.maximum(values, -most), most).astype(kind)


def setup_inputs(seed: int = 0) -> dict:
    seeds = jax.random.split(jax.random.key(seed), 4)
    return {
        "values": bell_draw(seeds[0], (ROWS, M), 1.0, 6.0, ((0, 512),), jnp.float32),
        "group_ids": draw_group_ids(jax.random.fold_in(seeds[3], 71), 0),
        "slot_of": jax.random.permutation(seeds[2], G).astype(jnp.int32),
    }


def block_pass(values, slots, groups):
    total_rows, width = values.shape
    size = math.gcd(total_rows, 256)
    blocks = total_rows // size
    lower = jnp.arange(size)[:, None] >= jnp.arange(size)[None, :]

    def advance(carry, item):
        sums, counts = carry
        rows, keys = item
        mask = ((keys[:, None] == keys[None, :]) & lower).astype(jnp.float32)
        within = jnp.dot(mask, rows, precision=lax.Precision.HIGHEST, preferred_element_type=jnp.float32)
        inclusive = within + jnp.take(sums, keys, axis=0)
        tally = jnp.sum(mask, axis=1) + jnp.take(counts, keys)
        sums = sums + jax.ops.segment_sum(rows, keys, num_segments=groups)
        counts = counts + jax.ops.segment_sum(jnp.ones((size,), jnp.float32), keys, num_segments=groups)
        return (sums, counts), (inclusive, tally)

    start = (jnp.zeros((groups, width), jnp.float32), jnp.zeros((groups,), jnp.float32))
    final, outs = lax.scan(advance, start, (values.reshape(blocks, size, width), slots.reshape(blocks, size)))
    return final, outs[0].reshape(total_rows, width), outs[1].reshape(total_rows)


def reference(values, group_ids, slot_of):
    slots = jnp.take(slot_of, group_ids).astype(jnp.int32)
    final, running_sum, count = block_pass(values, slots, G)
    running_mean = running_sum / count[:, None]
    closing_mean = final[0] / jnp.maximum(final[1], 1.0)[:, None]
    return running_mean, count.astype(jnp.int32), closing_mean
```

```python
import jax
import jax.numpy as jnp
from jax import lax
from jax.experimental import pallas as pl
from jax.experimental.pallas import tpu as pltpu
from jax.sharding import Mesh
from jax.sharding import PartitionSpec as P

ROWS_ALL = ("y", "z", "c", "x")
F32 = jnp.float32
BF16 = jnp.bfloat16
M = 64
R = 2048
S = 2048
LANES = 128
T = 256
NT = S // T
SIB = 8
FAR = 64
MSG = 136
LHS = 208


def pieces(v):
    a = v.astype(BF16)
    rest = v - a.astype(F32)
    b = rest.astype(BF16)
    c = (rest - b.astype(F32)).astype(BF16)
    return a, b, c


def lookup(table, idx):
    low = jnp.bitwise_and(idx, LANES - 1)
    high = jnp.right_shift(idx, 7)
    out = jnp.zeros_like(idx)
    for k in range(S // LANES):
        row = jnp.broadcast_to(table[k : k + 1, :], idx.shape)
        out = jnp.where(high == k, jnp.take_along_axis(row, low, axis=1), out)
    return out


def columns(slot):
    flipped = jnp.concatenate([slot] * 8, axis=0).T
    return [jnp.broadcast_to(flipped[:, i : i + 1], (LANES, LANES)) for i in range(R // LANES)]


def dot(a, b):
    return lax.dot_general(a, b, (((1,), (0,)), ((), ())), preferred_element_type=F32)


def sums_kernel(vt, gid, table, out, slot_out, cols, left, hot):
    slot = lookup(table[...], gid[...])
    slot_out[...] = slot
    for i, block in enumerate(columns(slot)):
        cols[i * LANES : (i + 1) * LANES, :] = block
    a, b, c = pieces(vt[...])
    left[0:64, :] = a
    left[64:128, :] = b
    left[128:192, :] = c
    left[192:208, :] = jnp.ones((16, R), BF16)
    lane = lax.broadcasted_iota(jnp.int32, (R, LANES), 1)
    first = lax.broadcasted_iota(jnp.int32, (8, LANES), 0) == 0

    def tile(j, carry):
        keys = cols[...] - lane
        for h in range(2):
            hot[:, h * LANES : (h + 1) * LANES] = jnp.where(
                keys == j * T + h * LANES, 1.0, 0.0
            ).astype(BF16)
        res = dot(left[...], hot[...])
        total = res[0:64] + (res[64:128] + res[128:192])
        out[j, 0:64, :] = total[:, :LANES]
        out[j, 64:128, :] = total[:, LANES:]
        out[j, 128:136, :] = jnp.where(first, res[192:200, :LANES], res[192:200, LANES:])
        return carry

    lax.fori_loop(0, NT, tile, 0)


def slice_kernel(arrived, out, buf):
    total = arrived[0]
    for i in range(1, SIB):
        total = total + arrived[i]
    buf[...] = total
    counts = buf[128:130, :]
    for p in range(FAR):
        out[p, 0:2, :] = buf[2 * p : 2 * p + 2, :]
        out[p, 2:4, :] = counts


def scan_kernel(place, arrived, out, counts_out):
    mine = place[0]
    acc = jnp.zeros((4, LANES), F32)
    before = jnp.zeros((4, LANES), F32)
    for p in range(FAR):
        got = arrived[p]
        out[p, 0:2, :] = acc[0:2]
        before = before + jnp.where(p < mine, got, 0.0)
        acc = acc + got
    number = jnp.where(mine < FAR // 2, acc[2:3], acc[3:4])
    closing = acc[0:2] / jnp.maximum(number, 1.0)
    for p in range(FAR):
        out[p, 2:4, :] = closing
    counts_out[0:2, :] = before[2:4]


def start_kernel(far, arrived, counts, out, closing, buf):
    for p in range(FAR):
        buf[2 * p : 2 * p + 2, :] = far[p, 0:2, :]
        closing[2 * p : 2 * p + 2, :] = far[p, 2:4, :]
    buf[128:130, :] = counts[0:2, :]
    buf[130:136, :] = jnp.zeros((6, LANES), F32)
    acc = buf[...]
    for k in range(SIB):
        i = 2 * (k % 4) + k // 4
        out[i] = acc
        acc = acc + arrived[i]


def running_kernel(start, vt, slot, closed, mean, count, closing, cols, left, local, hot, same):
    for i, block in enumerate(columns(slot[...])):
        cols[i * LANES : (i + 1) * LANES, :] = block
    a, b, c = pieces(vt[...])
    local[0:64, :] = a
    local[64:128, :] = b
    local[128:192, :] = c
    sub = lax.broadcasted_iota(jnp.int32, (16, R), 0)
    local[192:208, :] = jnp.where(sub == 0, 1.0, 0.0).astype(BF16)
    sub = lax.broadcasted_iota(jnp.int32, (16, LANES), 0)
    for j in range(NT):
        for h in range(2):
            at = slice(j * T + h * LANES, j * T + (h + 1) * LANES)
            a, b, c = pieces(start[j, h * 64 : (h + 1) * 64, :])
            left[0:64, at] = a
            left[64:128, at] = b
            left[128:192, at] = c
            a, b, c = (
                jnp.broadcast_to(v.astype(F32), (16, LANES))
                for v in pieces(start[j, 128 + h : 129 + h, :])
            )
            left[192:208, at] = jnp.where(
                sub == 0, a, jnp.where(sub == 1, b, jnp.where(sub == 2, c, 0.0))
            ).astype(BF16)
    for j in range(NT):
        upto = (j + 1) * T
        for h in range(2):
            i = 2 * j + h
            at = slice(h * LANES, (h + 1) * LANES)
            row = slot[i : i + 1, :]
            label = lax.broadcasted_iota(jnp.int32, (S, LANES), 0)
            hot[:, at] = jnp.where(label == row, 1.0, 0.0).astype(BF16)
            eq = cols[0:upto, :] == row
            if j:
                same[0 : j * T, at] = jnp.where(eq[0 : j * T], 1.0, 0.0).astype(BF16)
            q = lax.broadcasted_iota(jnp.int32, (T, LANES), 0)
            r = lax.broadcasted_iota(jnp.int32, (T, LANES), 1) + h * LANES
            last = jnp.logical_and(cols[j * T : upto, :] == row, q <= r)
            same[j * T : upto, at] = jnp.where(last, 1.0, 0.0).astype(BF16)
        res = dot(left[...], hot[...]) + dot(local[:, 0:upto], same[0:upto, :])
        total = res[0:64] + (res[64:128] + res[128:192])
        tally = (res[192:193] + res[193:194]) + res[194:195]
        mean[:, j * T : upto] = total / tally
        whole = tally.astype(jnp.int32)
        count[2 * j : 2 * j + 1, :] = whole[:, :LANES]
        count[2 * j + 1 : 2 * j + 2, :] = whole[:, LANES:]
    for c in range(2):
        for h in range(2):
            closing[:, c * T + h * LANES : c * T + (h + 1) * LANES] = closed[c, h * 64 : (h + 1) * 64, :]


def shape(*dims, dtype=F32):
    return jax.ShapeDtypeStruct(dims, dtype)


def sums_call(vt, gid, table):
    return pl.pallas_call(
        sums_kernel,
        out_shape=(shape(SIB, MSG, LANES), shape(16, LANES, dtype=jnp.int32)),
        scratch_shapes=[
            pltpu.VMEM((R, LANES), jnp.int32),
            pltpu.VMEM((LHS, R), BF16),
            pltpu.VMEM((R, T), BF16),
        ],
        name="local_sums",
    )(vt, gid, table)


def running_call(start, vt, slot, closed):
    return pl.pallas_call(
        running_kernel,
        out_shape=(shape(M, R), shape(16, LANES, dtype=jnp.int32), shape(M, 512)),
        scratch_shapes=[
            pltpu.VMEM((R, LANES), jnp.int32),
            pltpu.VMEM((LHS, S), BF16),
            pltpu.VMEM((LHS, R), BF16),
            pltpu.VMEM((S, T), BF16),
            pltpu.VMEM((R, T), BF16),
        ],
        name="running_means",
    )(start, vt, slot, closed)


def local(values, group_ids, slot_of):
    vt = values.T
    gid = group_ids.reshape(16, LANES)
    table = slot_of.reshape(16, LANES)
    sums, slot = sums_call(vt, gid, table)
    siblings = ("x", "c")
    far = ("y", "z")
    arrived = lax.all_to_all(sums, siblings, 0, 0, tiled=True)
    pieces_out = pl.pallas_call(
        slice_kernel,
        out_shape=shape(FAR, 4, LANES),
        scratch_shapes=[pltpu.VMEM((MSG, LANES), F32)],
        name="slice_sums",
    )(arrived)
    met = lax.all_to_all(pieces_out, far, 0, 0, tiled=True)
    place = (lax.axis_index("y") * 8 + lax.axis_index("z")).astype(jnp.int32).reshape(1)
    scanned, counts = pl.pallas_call(
        scan_kernel,
        in_specs=[
            pl.BlockSpec(memory_space=pltpu.SMEM),
            pl.BlockSpec(memory_space=pltpu.VMEM),
        ],
        out_shape=(shape(FAR, 4, LANES), shape(8, LANES)),
        name="scan",
    )(place, met)
    back = lax.all_to_all(scanned, far, 0, 0, tiled=True)
    starts, closing_half = pl.pallas_call(
        start_kernel,
        out_shape=(shape(SIB, MSG, LANES), shape(LANES, LANES)),
        scratch_shapes=[pltpu.VMEM((MSG, LANES), F32)],
        name="starts",
    )(back, arrived, counts)
    closed = lax.all_gather(closing_half, "c")
    start = lax.all_to_all(starts, siblings, 0, 0, tiled=True)
    mean, count, closing = running_call(start, vt, slot, closed)
    return mean.T, count.reshape(R), closing.T


def solution(mesh):
    split = Mesh(mesh.devices.reshape(8, 8, 2, 4), ROWS_ALL)
    in_specs = (P(ROWS_ALL, None), P(ROWS_ALL), P())
    out_specs = (P(ROWS_ALL, None), P(ROWS_ALL), P("x", None))
    return jax.shard_map(local, mesh=split, in_specs=in_specs, out_specs=out_specs, check_vma=False)
```

```python
import jax
import jax.numpy as jnp
from jax import lax
from jax.experimental import pallas as pl
from jax.experimental.pallas import tpu as pltpu
from jax.sharding import Mesh
from jax.sharding import PartitionSpec as P

ROWS_ALL = ("y", "z", "c", "x")
F32 = jnp.float32
BF16 = jnp.bfloat16
M = 64
R = 2048
S = 2048
LANES = 128
T = 256
NT = S // T
SIB = 8
FAR = 64
MSG = 136
LHS = 208


def pieces(v):
    a = v.astype(BF16)
    rest = v - a.astype(F32)
    b = rest.astype(BF16)
    c = (rest - b.astype(F32)).astype(BF16)
    return a, b, c


def lookup(table, idx):
    low = jnp.bitwise_and(idx, LANES - 1)
    high = jnp.right_shift(idx, 7)
    out = jnp.zeros_like(idx)
    for k in range(S // LANES):
        row = jnp.broadcast_to(table[k : k + 1, :], idx.shape)
        out = jnp.where(high == k, jnp.take_along_axis(row, low, axis=1), out)
    return out


def columns(slot):
    flipped = jnp.concatenate([slot] * 8, axis=0).T
    return [jnp.broadcast_to(flipped[:, i : i + 1], (LANES, LANES)) for i in range(R // LANES)]


def dot(a, b):
    return lax.dot_general(a, b, (((1,), (0,)), ((), ())), preferred_element_type=F32)


def sums_kernel(vt, gid, table, out, slot_out, cols, left, hot):
    slot = lookup(table[...], gid[...])
    slot_out[...] = slot
    for i, block in enumerate(columns(slot)):
        cols[i * LANES : (i + 1) * LANES, :] = block
    a, b, c = pieces(vt[...])
    left[0:64, :] = a
    left[64:128, :] = b
    left[128:192, :] = c
    left[192:208, :] = jnp.ones((16, R), BF16)
    lane = lax.broadcasted_iota(jnp.int32, (R, LANES), 1)
    first = lax.broadcasted_iota(jnp.int32, (8, LANES), 0) == 0

    def tile(j, carry):
        keys = cols[...] - lane
        for h in range(2):
            hot[:, h * LANES : (h + 1) * LANES] = jnp.where(
                keys == j * T + h * LANES, 1.0, 0.0
            ).astype(BF16)
        res = dot(left[...], hot[...])
        total = res[0:64] + (res[64:128] + res[128:192])
        out[j, 0:64, :] = total[:, :LANES]
        out[j, 64:128, :] = total[:, LANES:]
        out[j, 128:136, :] = jnp.where(first, res[192:200, :LANES], res[192:200, LANES:])
        return carry

    lax.fori_loop(0, NT, tile, 0)


def slice_kernel(arrived, out, buf):
    total = arrived[0]
    for i in range(1, SIB):
        total = total + arrived[i]
    buf[...] = total
    counts = buf[128:130, :]
    for p in range(FAR):
        out[p, 0:2, :] = buf[2 * p : 2 * p + 2, :]
        out[p, 2:4, :] = counts


def scan_kernel(arrived, out, counts_out):
    mine = lax.axis_index("y") * 8 + lax.axis_index("z")
    acc = jnp.zeros((4, LANES), F32)
    before = jnp.zeros((4, LANES), F32)
    for p in range(FAR):
        got = arrived[p]
        out[p, 0:2, :] = acc[0:2]
        before = before + jnp.where(p < mine, got, 0.0)
        acc = acc + got
    number = jnp.where(mine < FAR // 2, acc[2:3], acc[3:4])
    closing = acc[0:2] / jnp.maximum(number, 1.0)
    for p in range(FAR):
        out[p, 2:4, :] = closing
    counts_out[0:2, :] = before[2:4]


def start_kernel(far, arrived, counts, out, closing, buf):
    for p in range(FAR):
        buf[2 * p : 2 * p + 2, :] = far[p, 0:2, :]
        closing[2 * p : 2 * p + 2, :] = far[p, 2:4, :]
    buf[128:130, :] = counts[0:2, :]
    buf[130:136, :] = jnp.zeros((6, LANES), F32)
    acc = buf[...]
    for k in range(SIB):
        i = 2 * (k % 4) + k // 4
        out[i] = acc
        acc = acc + arrived[i]


def running_kernel(start, vt, slot, closed, mean, count, closing, cols, left, local, hot, same):
    for i, block in enumerate(columns(slot[...])):
        cols[i * LANES : (i + 1) * LANES, :] = block
    a, b, c = pieces(vt[...])
    local[0:64, :] = a
    local[64:128, :] = b
    local[128:192, :] = c
    sub = lax.broadcasted_iota(jnp.int32, (16, R), 0)
    local[192:208, :] = jnp.where(sub == 0, 1.0, 0.0).astype(BF16)
    sub = lax.broadcasted_iota(jnp.int32, (16, LANES), 0)
    for j in range(NT):
        for h in range(2):
            at = slice(j * T + h * LANES, j * T + (h + 1) * LANES)
            a, b, c = pieces(start[j, h * 64 : (h + 1) * 64, :])
            left[0:64, at] = a
            left[64:128, at] = b
            left[128:192, at] = c
            a, b, c = (
                jnp.broadcast_to(v.astype(F32), (16, LANES))
                for v in pieces(start[j, 128 + h : 129 + h, :])
            )
            left[192:208, at] = jnp.where(
                sub == 0, a, jnp.where(sub == 1, b, jnp.where(sub == 2, c, 0.0))
            ).astype(BF16)
    for j in range(NT):
        upto = (j + 1) * T
        for h in range(2):
            i = 2 * j + h
            at = slice(h * LANES, (h + 1) * LANES)
            row = slot[i : i + 1, :]
            label = lax.broadcasted_iota(jnp.int32, (S, LANES), 0)
            hot[:, at] = jnp.where(label == row, 1.0, 0.0).astype(BF16)
            eq = cols[0:upto, :] == row
            if j:
                same[0 : j * T, at] = jnp.where(eq[0 : j * T], 1.0, 0.0).astype(BF16)
            q = lax.broadcasted_iota(jnp.int32, (T, LANES), 0)
            r = lax.broadcasted_iota(jnp.int32, (T, LANES), 1) + h * LANES
            last = jnp.logical_and(cols[j * T : upto, :] == row, q <= r)
            same[j * T : upto, at] = jnp.where(last, 1.0, 0.0).astype(BF16)
        res = dot(left[...], hot[...]) + dot(local[:, 0:upto], same[0:upto, :])
        total = res[0:64] + (res[64:128] + res[128:192])
        tally = (res[192:193] + res[193:194]) + res[194:195]
        mean[:, j * T : upto] = total / tally
        whole = tally.astype(jnp.int32)
        count[2 * j : 2 * j + 1, :] = whole[:, :LANES]
        count[2 * j + 1 : 2 * j + 2, :] = whole[:, LANES:]
    for c in range(2):
        for h in range(2):
            closing[:, c * T + h * LANES : c * T + (h + 1) * LANES] = closed[c, h * 64 : (h + 1) * 64, :]


def shape(*dims, dtype=F32):
    return jax.ShapeDtypeStruct(dims, dtype)


def near(*dims, dtype=F32):
    return pltpu.VMEM(dims, dtype)


def held(x):
    return pltpu.with_memory_space_constraint(x, pltpu.VMEM)


def sums_call(vt, gid, table):
    return pl.pallas_call(
        sums_kernel,
        out_shape=(near(SIB, MSG, LANES), near(16, LANES, dtype=jnp.int32)),
        scratch_shapes=[
            pltpu.VMEM((R, LANES), jnp.int32),
            pltpu.VMEM((LHS, R), BF16),
            pltpu.VMEM((R, T), BF16),
        ],
        name="local_sums",
    )(vt, gid, table)


def running_call(start, vt, slot, closed):
    return pl.pallas_call(
        running_kernel,
        out_shape=(shape(M, R), shape(16, LANES, dtype=jnp.int32), shape(M, 512)),
        scratch_shapes=[
            pltpu.VMEM((R, LANES), jnp.int32),
            pltpu.VMEM((LHS, S), BF16),
            pltpu.VMEM((LHS, R), BF16),
            pltpu.VMEM((S, T), BF16),
            pltpu.VMEM((R, T), BF16),
        ],
        name="running_means",
    )(start, vt, slot, closed)


def local(values, group_ids, slot_of):
    vt = values.T
    gid = group_ids.reshape(16, LANES)
    table = slot_of.reshape(16, LANES)
    sums, slot = sums_call(vt, gid, table)
    siblings = ("x", "c")
    far = ("y", "z")
    arrived = held(lax.all_to_all(sums, siblings, 0, 0, tiled=True))
    pieces_out = pl.pallas_call(
        slice_kernel,
        out_shape=near(FAR, 4, LANES),
        scratch_shapes=[pltpu.VMEM((MSG, LANES), F32)],
        name="slice_sums",
    )(arrived)
    met = held(lax.all_to_all(pieces_out, far, 0, 0, tiled=True))
    scanned, counts = pl.pallas_call(
        scan_kernel,
        out_shape=(near(FAR, 4, LANES), near(8, LANES)),
        name="scan",
    )(met)
    back = held(lax.all_to_all(scanned, far, 0, 0, tiled=True))
    starts, closing_half = pl.pallas_call(
        start_kernel,
        out_shape=(near(SIB, MSG, LANES), near(LANES, LANES)),
        scratch_shapes=[pltpu.VMEM((MSG, LANES), F32)],
        name="starts",
    )(back, arrived, counts)
    closed = lax.all_gather(closing_half, "c")
    starts, closed = lax.optimization_barrier((starts, closed))
    closed = held(closed)
    start = held(lax.all_to_all(starts, siblings, 0, 0, tiled=True))
    mean, count, closing = running_call(start, vt, slot, closed)
    return mean.T, count.reshape(R), closing.T


def solution(mesh):
    split = Mesh(mesh.devices.reshape(8, 8, 2, 4), ROWS_ALL)
    in_specs = (P(ROWS_ALL, None), P(ROWS_ALL), P())
    out_specs = (P(ROWS_ALL, None), P(ROWS_ALL), P("x", None))
    return jax.shard_map(local, mesh=split, in_specs=in_specs, out_specs=out_specs, check_vma=False)
```

```python
import jax
import jax.numpy as jnp
from jax import lax
from jax.experimental import pallas as pl
from jax.experimental.pallas import tpu as pltpu
from jax.sharding import Mesh
from jax.sharding import PartitionSpec as P

ROWS_ALL = ("y", "z", "c", "x")
F32 = jnp.float32
BF16 = jnp.bfloat16
M = 64
R = 2048
S = 2048
LANES = 128
T = 256
NT = S // T
SIB = 8
FAR = 64
MSG = 136
LHS = 208


ROOM = pltpu.CompilerParams(vmem_limit_bytes=16 << 20)


def pieces(v):
    a = v.astype(BF16)
    rest = v - a.astype(F32)
    b = rest.astype(BF16)
    c = (rest - b.astype(F32)).astype(BF16)
    return a, b, c


def lookup(table, idx):
    low = jnp.bitwise_and(idx, LANES - 1)
    high = jnp.right_shift(idx, 7)
    out = jnp.zeros_like(idx)
    for k in range(S // LANES):
        row = jnp.broadcast_to(table[k : k + 1, :], idx.shape)
        out = jnp.where(high == k, jnp.take_along_axis(row, low, axis=1), out)
    return out


def columns(slot):
    flipped = jnp.concatenate([slot] * 8, axis=0).T
    return [jnp.broadcast_to(flipped[:, i : i + 1], (LANES, LANES)) for i in range(R // LANES)]


def dot(a, b):
    return lax.dot_general(a, b, (((1,), (0,)), ((), ())), preferred_element_type=F32)


def hot(mask):
    return jnp.where(mask, 1.0, 0.0).astype(BF16)


def sums_kernel(vt_far, gid_far, table_far, out, slot_out, local, cols, vt, gid, table, sems):
    values_in = pltpu.make_async_copy(vt_far, vt, sems.at[0])
    keys_in = pltpu.make_async_copy(gid_far, gid, sems.at[1])
    table_in = pltpu.make_async_copy(table_far, table, sems.at[2])
    keys_in.start()
    table_in.start()
    values_in.start()
    keys_in.wait()
    table_in.wait()
    slot = lookup(table[...], gid[...])
    slot_out[...] = slot
    for i, block in enumerate(columns(slot)):
        cols[i * LANES : (i + 1) * LANES, :] = block
    values_in.wait()
    a, b, c = pieces(vt[...])
    local[0:64, :] = a
    local[64:128, :] = b
    local[128:192, :] = c
    sub = lax.broadcasted_iota(jnp.int32, (16, R), 0)
    local[192:208, :] = jnp.where(sub == 0, 1.0, 0.0).astype(BF16)
    lane = lax.broadcasted_iota(jnp.int32, (T, T), 1)
    first = lax.broadcasted_iota(jnp.int32, (8, LANES), 0) == 0
    for j in range(NT):
        res = None
        for k in range(NT):
            at = slice(k * T, (k + 1) * T)
            keys = cols[at, :]
            keys = jnp.concatenate([keys, keys], axis=1)
            part = dot(local[:, at], hot(keys == lane + j * T))
            res = part if res is None else res + part
        total = res[0:64] + (res[64:128] + res[128:192])
        out[j, 0:64, :] = total[:, :LANES]
        out[j, 64:128, :] = total[:, LANES:]
        number = jnp.broadcast_to(res[192:193], (8, T))
        out[j, 128:136, :] = jnp.where(first, number[:, :LANES], number[:, LANES:])


def slice_kernel(arrived, out, buf):
    total = arrived[0]
    for i in range(1, SIB):
        total = total + arrived[i]
    buf[...] = total
    counts = buf[128:130, :]
    for p in range(FAR):
        out[p, 0:2, :] = buf[2 * p : 2 * p + 2, :]
        out[p, 2:4, :] = counts


def scan_kernel(arrived, out, counts_out):
    mine = lax.axis_index("y") * 8 + lax.axis_index("z")
    acc = jnp.zeros((4, LANES), F32)
    before = jnp.zeros((4, LANES), F32)
    for p in range(FAR):
        got = arrived[p]
        out[p, 0:2, :] = acc[0:2]
        before = before + jnp.where(p < mine, got, 0.0)
        acc = acc + got
    number = jnp.where(mine < FAR // 2, acc[2:3], acc[3:4])
    closing = acc[0:2] / jnp.maximum(number, 1.0)
    for p in range(FAR):
        out[p, 2:4, :] = closing
    counts_out[0:2, :] = before[2:4]


def start_kernel(far, arrived, counts, out, closing, buf):
    for p in range(FAR):
        buf[2 * p : 2 * p + 2, :] = far[p, 0:2, :]
        closing[2 * p : 2 * p + 2, :] = far[p, 2:4, :]
    buf[128:130, :] = counts[0:2, :]
    buf[130:136, :] = jnp.zeros((6, LANES), F32)
    acc = buf[...]
    for k in range(SIB):
        i = 2 * (k % 4) + k // 4
        out[i] = acc
        acc = acc + arrived[i]


def running_kernel(start, local, slot, cols, closed, mean, count, closing, left, held_mean, sems):
    sub = lax.broadcasted_iota(jnp.int32, (16, LANES), 0)
    for j in range(NT):
        for h in range(2):
            at = slice(j * T + h * LANES, j * T + (h + 1) * LANES)
            a, b, c = pieces(start[j, h * 64 : (h + 1) * 64, :])
            left[0:64, at] = a
            left[64:128, at] = b
            left[128:192, at] = c
            a, b, c = (
                jnp.broadcast_to(v.astype(F32), (16, LANES))
                for v in pieces(start[j, 128 + h : 129 + h, :])
            )
            left[192:208, at] = jnp.where(
                sub == 0, a, jnp.where(sub == 1, b, jnp.where(sub == 2, c, 0.0))
            ).astype(BF16)
    label = lax.broadcasted_iota(jnp.int32, (T, T), 0)
    order = label <= lax.broadcasted_iota(jnp.int32, (T, T), 1)
    copies = []
    for j in range(NT):
        row = jnp.concatenate([slot[2 * j : 2 * j + 1, :], slot[2 * j + 1 : 2 * j + 2, :]], axis=1)
        row = jnp.broadcast_to(row, (T, T))
        res = None
        for k in range(NT):
            part = dot(left[:, k * T : (k + 1) * T], hot(label + k * T == row))
            res = part if res is None else res + part
        for k in range(j + 1):
            at = slice(k * T, (k + 1) * T)
            keys = cols[at, :]
            mask = jnp.concatenate([keys, keys], axis=1) == row
            if k == j:
                mask = jnp.logical_and(mask, order)
            res = res + dot(local[:, at], hot(mask))
        total = res[0:64] + (res[64:128] + res[128:192])
        tally = (res[192:193] + res[193:194]) + res[194:195]
        at = slice(j * T, (j + 1) * T)
        held_mean[:, at] = total / tally
        copies.append(pltpu.make_async_copy(held_mean.at[:, at], mean.at[:, at], sems.at[j]))
        copies[-1].start()
        whole = tally.astype(jnp.int32)
        count[2 * j : 2 * j + 1, :] = whole[:, :LANES]
        count[2 * j + 1 : 2 * j + 2, :] = whole[:, LANES:]
    for c in range(2):
        for h in range(2):
            closing[:, c * T + h * LANES : c * T + (h + 1) * LANES] = closed[c, h * 64 : (h + 1) * 64, :]
    for copy in copies:
        copy.wait()


def shape(*dims, dtype=F32):
    return jax.ShapeDtypeStruct(dims, dtype)


def near(*dims, dtype=F32):
    return pltpu.VMEM(dims, dtype)


def outer(x):
    return pltpu.with_memory_space_constraint(x, pltpu.HBM)


def held(x):
    return pltpu.with_memory_space_constraint(x, pltpu.VMEM)


def sums_call(vt, gid, table):
    outside = pl.BlockSpec(memory_space=pl.ANY)
    return pl.pallas_call(
        sums_kernel,
        in_specs=[outside] * 3,
        out_shape=(
            near(SIB, MSG, LANES),
            near(16, LANES, dtype=jnp.int32),
            near(LHS, R, dtype=BF16),
            near(R, LANES, dtype=jnp.int32),
        ),
        scratch_shapes=[
            pltpu.VMEM((M, R), F32),
            pltpu.VMEM((16, LANES), jnp.int32),
            pltpu.VMEM((16, LANES), jnp.int32),
            pltpu.SemaphoreType.DMA((3,)),
        ],
        compiler_params=ROOM,
        name="local_sums",
    )(outer(vt), outer(gid), outer(table))


def running_call(start, local, slot, cols, closed):
    vmem = pl.BlockSpec(memory_space=pltpu.VMEM)
    return pl.pallas_call(
        running_kernel,
        out_shape=(shape(M, R), shape(16, LANES, dtype=jnp.int32), shape(M, 512)),
        out_specs=(pl.BlockSpec(memory_space=pl.ANY), vmem, vmem),
        scratch_shapes=[
            pltpu.VMEM((LHS, S), BF16),
            pltpu.VMEM((M, R), F32),
            pltpu.SemaphoreType.DMA((NT,)),
        ],
        compiler_params=ROOM,
        name="running_means",
    )(start, held(local), held(slot), held(cols), closed)


def local(values, group_ids, slot_of):
    vt = values.T
    gid = group_ids.reshape(16, LANES)
    table = slot_of.reshape(16, LANES)
    sums, slot, local_pieces, cols = sums_call(vt, gid, table)
    siblings = ("x", "c")
    far = ("y", "z")
    arrived = held(lax.all_to_all(sums, siblings, 0, 0, tiled=True))
    pieces_out = pl.pallas_call(
        slice_kernel,
        out_shape=near(FAR, 4, LANES),
        scratch_shapes=[pltpu.VMEM((MSG, LANES), F32)],
        compiler_params=ROOM,
        name="slice_sums",
    )(arrived)
    met = held(lax.all_to_all(pieces_out, far, 0, 0, tiled=True))
    scanned, counts = pl.pallas_call(
        scan_kernel,
        out_shape=(near(FAR, 4, LANES), near(8, LANES)),
        compiler_params=ROOM,
        name="scan",
    )(met)
    back = held(lax.all_to_all(scanned, far, 0, 0, tiled=True))
    starts, closing_half = pl.pallas_call(
        start_kernel,
        out_shape=(near(SIB, MSG, LANES), near(LANES, LANES)),
        scratch_shapes=[pltpu.VMEM((MSG, LANES), F32)],
        compiler_params=ROOM,
        name="starts",
    )(back, arrived, counts)
    closed = lax.all_gather(closing_half, "c")
    starts, closed = lax.optimization_barrier((starts, closed))
    closed = held(closed)
    start = held(lax.all_to_all(starts, siblings, 0, 0, tiled=True))
    mean, count, closing = running_call(start, local_pieces, slot, cols, closed)
    return mean.T, count.reshape(R), closing.T


def solution(mesh):
    split = Mesh(mesh.devices.reshape(8, 8, 2, 4), ROWS_ALL)
    in_specs = (P(ROWS_ALL, None), P(ROWS_ALL), P())
    out_specs = (P(ROWS_ALL, None), P(ROWS_ALL), P("x", None))
    return jax.shard_map(local, mesh=split, in_specs=in_specs, out_specs=out_specs, check_vma=False)
```

```python
import jax
import jax.numpy as jnp
from jax import lax
from jax.experimental import pallas as pl
from jax.experimental.pallas import tpu as pltpu
from jax.sharding import Mesh
from jax.sharding import PartitionSpec as P

ROWS_ALL = ("y", "z", "c", "x")
F32 = jnp.float32
BF16 = jnp.bfloat16
M = 64
R = 2048
S = 2048
LANES = 128
T = 256
NT = S // T
SIB = 8
RING = 8
MSG = 136
LHS = 208


ROOM = pltpu.CompilerParams(vmem_limit_bytes=16 << 20)


def pieces(v):
    a = v.astype(BF16)
    rest = v - a.astype(F32)
    b = rest.astype(BF16)
    c = (rest - b.astype(F32)).astype(BF16)
    return a, b, c


def lookup(table, idx):
    low = jnp.bitwise_and(idx, LANES - 1)
    high = jnp.right_shift(idx, 7)
    out = jnp.zeros_like(idx)
    for k in range(S // LANES):
        row = jnp.broadcast_to(table[k : k + 1, :], idx.shape)
        out = jnp.where(high == k, jnp.take_along_axis(row, low, axis=1), out)
    return out


def columns(slot):
    flipped = jnp.concatenate([slot] * 8, axis=0).T
    return [jnp.broadcast_to(flipped[:, i : i + 1], (LANES, LANES)) for i in range(R // LANES)]


def dot(a, b):
    return lax.dot_general(a, b, (((1,), (0,)), ((), ())), preferred_element_type=F32)


def hot(mask):
    return jnp.where(mask, 1.0, 0.0).astype(BF16)


def sums_kernel(vt_far, gid_far, table_far, out, slot_out, local, cols, vt, gid, table, sems):
    values_in = pltpu.make_async_copy(vt_far, vt, sems.at[0])
    keys_in = pltpu.make_async_copy(gid_far, gid, sems.at[1])
    table_in = pltpu.make_async_copy(table_far, table, sems.at[2])
    keys_in.start()
    table_in.start()
    values_in.start()
    keys_in.wait()
    table_in.wait()
    slot = lookup(table[...], gid[...])
    slot_out[...] = slot
    for i, block in enumerate(columns(slot)):
        cols[i * LANES : (i + 1) * LANES, :] = block
    values_in.wait()
    a, b, c = pieces(vt[...])
    local[0:64, :] = a
    local[64:128, :] = b
    local[128:192, :] = c
    sub = lax.broadcasted_iota(jnp.int32, (16, R), 0)
    local[192:208, :] = jnp.where(sub == 0, 1.0, 0.0).astype(BF16)
    lane = lax.broadcasted_iota(jnp.int32, (T, T), 1)
    first = lax.broadcasted_iota(jnp.int32, (8, LANES), 0) == 0
    for j in range(NT):
        res = None
        for k in range(NT):
            at = slice(k * T, (k + 1) * T)
            keys = cols[at, :]
            keys = jnp.concatenate([keys, keys], axis=1)
            part = dot(local[:, at], hot(keys == lane + j * T))
            res = part if res is None else res + part
        total = res[0:64] + (res[64:128] + res[128:192])
        out[j, 0:64, :] = total[:, :LANES]
        out[j, 64:128, :] = total[:, LANES:]
        number = jnp.broadcast_to(res[192:193], (8, T))
        out[j, 128:136, :] = jnp.where(first, number[:, :LANES], number[:, LANES:])


def slice_kernel(arrived, out):
    total = arrived[0]
    for i in range(1, SIB):
        total = total + arrived[i]
    for p in range(RING):
        out[p, 0:16, :] = total[16 * p : 16 * p + 16]
        out[p, 16:24, :] = total[128:136]


def ring_kernel(arrived, out):
    total = arrived[0]
    for i in range(1, RING):
        total = total + arrived[i]
    for p in range(RING):
        out[p] = total


def scan_kernel(arrived, rings, out, counts_out):
    y = lax.axis_index("y")
    z = lax.axis_index("z")
    total = rings[0]
    before = jnp.where(y > 0, total, 0.0)
    for i in range(1, RING):
        ring = rings[i]
        before = before + jnp.where(i < y, ring, 0.0)
        total = total + ring
    number = jnp.where(z < RING // 2, total[16:17], total[17:18])
    closing = total[0:16] / jnp.maximum(number, 1.0)
    counts = before[16:24]
    acc = before[0:16]
    for p in range(RING):
        out[p, 0:16, :] = acc
        out[p, 16:32, :] = closing
        acc = acc + arrived[p, 0:16, :]
        counts = counts + jnp.where(p < z, arrived[p, 16:24, :], 0.0)
    counts_out[...] = counts


def start_kernel(far, arrived, counts, out, closing):
    parts = []
    for p in range(RING):
        parts.append(far[p, 0:16, :])
        closing[16 * p : 16 * p + 16, :] = far[p, 16:32, :]
    acc = jnp.concatenate(parts + [counts[...]], axis=0)
    for k in range(SIB):
        i = 2 * (k % 4) + k // 4
        out[i] = acc
        acc = acc + arrived[i]


def running_kernel(start, local, slot, cols, closed, mean, count, closing, left, held_mean, sems):
    sub = lax.broadcasted_iota(jnp.int32, (16, LANES), 0)
    for j in range(NT):
        for h in range(2):
            at = slice(j * T + h * LANES, j * T + (h + 1) * LANES)
            a, b, c = pieces(start[j, h * 64 : (h + 1) * 64, :])
            left[0:64, at] = a
            left[64:128, at] = b
            left[128:192, at] = c
            a, b, c = (
                jnp.broadcast_to(v.astype(F32), (16, LANES))
                for v in pieces(start[j, 128 + h : 129 + h, :])
            )
            left[192:208, at] = jnp.where(
                sub == 0, a, jnp.where(sub == 1, b, jnp.where(sub == 2, c, 0.0))
            ).astype(BF16)
    label = lax.broadcasted_iota(jnp.int32, (T, T), 0)
    order = label <= lax.broadcasted_iota(jnp.int32, (T, T), 1)
    copies = []
    for j in range(NT):
        row = jnp.concatenate([slot[2 * j : 2 * j + 1, :], slot[2 * j + 1 : 2 * j + 2, :]], axis=1)
        row = jnp.broadcast_to(row, (T, T))
        res = None
        for k in range(NT):
            part = dot(left[:, k * T : (k + 1) * T], hot(label + k * T == row))
            res = part if res is None else res + part
        for k in range(j + 1):
            at = slice(k * T, (k + 1) * T)
            keys = cols[at, :]
            mask = jnp.concatenate([keys, keys], axis=1) == row
            if k == j:
                mask = jnp.logical_and(mask, order)
            res = res + dot(local[:, at], hot(mask))
        total = res[0:64] + (res[64:128] + res[128:192])
        tally = (res[192:193] + res[193:194]) + res[194:195]
        at = slice(j * T, (j + 1) * T)
        held_mean[:, at] = total / tally
        copies.append(pltpu.make_async_copy(held_mean.at[:, at], mean.at[:, at], sems.at[j]))
        copies[-1].start()
        whole = tally.astype(jnp.int32)
        count[2 * j : 2 * j + 1, :] = whole[:, :LANES]
        count[2 * j + 1 : 2 * j + 2, :] = whole[:, LANES:]
    for c in range(2):
        for h in range(2):
            closing[:, c * T + h * LANES : c * T + (h + 1) * LANES] = closed[c, h * 64 : (h + 1) * 64, :]
    for copy in copies:
        copy.wait()


def shape(*dims, dtype=F32):
    return jax.ShapeDtypeStruct(dims, dtype)


def near(*dims, dtype=F32):
    return pltpu.VMEM(dims, dtype)


def outer(x):
    return pltpu.with_memory_space_constraint(x, pltpu.HBM)


def held(x):
    return pltpu.with_memory_space_constraint(x, pltpu.VMEM)


def sums_call(vt, gid, table):
    outside = pl.BlockSpec(memory_space=pl.ANY)
    return pl.pallas_call(
        sums_kernel,
        in_specs=[outside] * 3,
        out_shape=(
            near(SIB, MSG, LANES),
            near(16, LANES, dtype=jnp.int32),
            near(LHS, R, dtype=BF16),
            near(R, LANES, dtype=jnp.int32),
        ),
        scratch_shapes=[
            pltpu.VMEM((M, R), F32),
            pltpu.VMEM((16, LANES), jnp.int32),
            pltpu.VMEM((16, LANES), jnp.int32),
            pltpu.SemaphoreType.DMA((3,)),
        ],
        compiler_params=ROOM,
        name="local_sums",
    )(outer(vt), outer(gid), outer(table))


def running_call(start, local, slot, cols, closed):
    vmem = pl.BlockSpec(memory_space=pltpu.VMEM)
    return pl.pallas_call(
        running_kernel,
        out_shape=(shape(M, R), shape(16, LANES, dtype=jnp.int32), shape(M, 512)),
        out_specs=(pl.BlockSpec(memory_space=pl.ANY), vmem, vmem),
        scratch_shapes=[
            pltpu.VMEM((LHS, S), BF16),
            pltpu.VMEM((M, R), F32),
            pltpu.SemaphoreType.DMA((NT,)),
        ],
        compiler_params=ROOM,
        name="running_means",
    )(start, held(local), held(slot), held(cols), closed)


def local(values, group_ids, slot_of):
    vt = values.T
    gid = group_ids.reshape(16, LANES)
    table = slot_of.reshape(16, LANES)
    sums, slot, local_pieces, cols = sums_call(vt, gid, table)
    siblings = ("x", "c")
    arrived = held(lax.all_to_all(sums, siblings, 0, 0, tiled=True))
    parts = pl.pallas_call(
        slice_kernel,
        out_shape=near(RING, 24, LANES),
        compiler_params=ROOM,
        name="slice_sums",
    )(arrived)
    along_z = held(lax.all_to_all(parts, "z", 0, 0, tiled=True))
    ring = pl.pallas_call(
        ring_kernel,
        out_shape=near(RING, 24, LANES),
        compiler_params=ROOM,
        name="ring_sums",
    )(along_z)
    along_y = held(lax.all_to_all(ring, "y", 0, 0, tiled=True))
    scanned, counts = pl.pallas_call(
        scan_kernel,
        out_shape=(near(RING, 32, LANES), near(8, LANES)),
        compiler_params=ROOM,
        name="scan",
    )(along_z, along_y)
    back = held(lax.all_to_all(scanned, "z", 0, 0, tiled=True))
    starts, closing_half = pl.pallas_call(
        start_kernel,
        out_shape=(near(SIB, MSG, LANES), near(LANES, LANES)),
        compiler_params=ROOM,
        name="starts",
    )(back, arrived, counts)
    closed = lax.all_gather(closing_half, "c")
    starts, closed = lax.optimization_barrier((starts, closed))
    closed = held(closed)
    start = held(lax.all_to_all(starts, siblings, 0, 0, tiled=True))
    mean, count, closing = running_call(start, local_pieces, slot, cols, closed)
    return mean.T, count.reshape(R), closing.T


def solution(mesh):
    split = Mesh(mesh.devices.reshape(8, 8, 2, 4), ROWS_ALL)
    in_specs = (P(ROWS_ALL, None), P(ROWS_ALL), P())
    out_specs = (P(ROWS_ALL, None), P(ROWS_ALL), P("x", None))
    return jax.shard_map(local, mesh=split, in_specs=in_specs, out_specs=out_specs, check_vma=False)
```

```python
import jax
import jax.numpy as jnp
from jax import lax
from jax.experimental import pallas as pl
from jax.experimental.pallas import tpu as pltpu
from jax.sharding import Mesh
from jax.sharding import PartitionSpec as P

ROWS_ALL = ("y", "z", "c", "x")
F32 = jnp.float32
BF16 = jnp.bfloat16
M = 64
R = 2048
S = 2048
LANES = 128
T = 256
NT = S // T
NH = NT // 2
SIB = 8
RING = 8
MSG = 136
LHS = 144
HALF = 1024


ROOM = pltpu.CompilerParams(vmem_limit_bytes=16 << 20)


def pieces(v):
    a = v.astype(BF16)
    rest = v - a.astype(F32)
    b = rest.astype(BF16)
    c = (rest - b.astype(F32)).astype(BF16)
    return a, b, c


def lookup(table, idx):
    low = jnp.bitwise_and(idx, LANES - 1)
    high = jnp.right_shift(idx, 7)
    out = jnp.zeros_like(idx)
    for k in range(S // LANES):
        row = jnp.broadcast_to(table[k : k + 1, :], idx.shape)
        out = jnp.where(high == k, jnp.take_along_axis(row, low, axis=1), out)
    return out


def columns(slot):
    flipped = jnp.concatenate([slot] * 8, axis=0).T
    return [jnp.broadcast_to(flipped[:, i : i + 1], (LANES, LANES)) for i in range(R // LANES)]


def dot(a, b):
    return lax.dot_general(a, b, (((1,), (0,)), ((), ())), preferred_element_type=F32)


def hot(mask):
    return jnp.where(mask, 1.0, 0.0).astype(BF16)


def sums_kernel(vt_far, gid_far, table_far, out, slot_out, local, cols, vt, gid, table, split, sems):
    values_in = [
        pltpu.make_async_copy(vt_far.at[16 * g : 16 * g + 16], vt.at[16 * g : 16 * g + 16], sems.at[3 + g]) for g in range(4)
    ]
    keys_in = pltpu.make_async_copy(gid_far, gid, sems.at[1])
    table_in = pltpu.make_async_copy(table_far, table, sems.at[2])
    keys_in.start()
    table_in.start()
    for copy in values_in:
        copy.start()
    keys_in.wait()
    table_in.wait()
    slot = lookup(table[...], gid[...])
    slot_out[...] = slot
    sub = lax.broadcasted_iota(jnp.int32, (16, LANES), 0)
    ones = jnp.where(sub == 0, 1.0, 0.0)
    spans = [slice(i * LANES, (i + 1) * LANES) for i in range(R // LANES)]
    highs = [jnp.broadcast_to(slot[i : i + 1, :], (16, LANES)) >= HALF for i in range(R // LANES)]

    def place(rows, value):
        for at, high in zip(spans, highs):
            v = value[:, at] if value.shape[1] > LANES else value
            local[rows : rows + 16, at] = v.astype(BF16)
            split[rows : rows + 16, at] = jnp.where(high, 0.0, v).astype(BF16)
            split[LHS + rows : LHS + rows + 16, at] = jnp.where(high, v, 0.0).astype(BF16)

    place(128, ones)
    for g in range(4):
        values_in[g].wait()
        a, b, _ = pieces(vt[16 * g : 16 * g + 16, :])
        place(16 * g, a.astype(F32))
        place(64 + 16 * g, b.astype(F32))
    for i, block in enumerate(columns(slot)):
        cols[i * LANES : (i + 1) * LANES, :] = block
    lane = lax.broadcasted_iota(jnp.int32, (T, T), 1)
    first = lax.broadcasted_iota(jnp.int32, (8, LANES), 0) == 0
    for j in range(NH):
        res = None
        for k in range(NT):
            at = slice(k * T, (k + 1) * T)
            keys = jnp.bitwise_and(cols[at, :], HALF - 1)
            keys = jnp.concatenate([keys, keys], axis=1)
            part = dot(split[:, at], hot(keys == lane + j * T))
            res = part if res is None else res + part
        for h in range(2):
            of = res[h * LHS : (h + 1) * LHS]
            total = of[0:64] + of[64:128]
            to = h * NH + j
            out[to, 0:64, :] = total[:, :LANES]
            out[to, 64:128, :] = total[:, LANES:]
            number = jnp.broadcast_to(of[128:129], (8, T))
            out[to, 128:136, :] = jnp.where(first, number[:, :LANES], number[:, LANES:])


def slice_kernel(arrived, out):
    total = arrived[0]
    for i in range(1, SIB):
        total = total + arrived[i]
    for p in range(RING):
        out[p, 0:16, :] = total[16 * p : 16 * p + 16]
        out[p, 16:24, :] = total[128:136]


def ring_kernel(arrived, out):
    total = arrived[0]
    for i in range(1, RING):
        total = total + arrived[i]
    for p in range(RING):
        out[p] = total


def scan_kernel(arrived, rings, out, counts_out):
    y = lax.axis_index("y")
    z = lax.axis_index("z")
    total = rings[0]
    before = jnp.where(y > 0, total, 0.0)
    for i in range(1, RING):
        ring = rings[i]
        before = before + jnp.where(i < y, ring, 0.0)
        total = total + ring
    number = jnp.where(z < RING // 2, total[16:17], total[17:18])
    closing = total[0:16] / jnp.maximum(number, 1.0)
    counts = before[16:24]
    acc = before[0:16]
    for p in range(RING):
        out[p, 0:16, :] = acc
        out[p, 16:32, :] = closing
        acc = acc + arrived[p, 0:16, :]
        counts = counts + jnp.where(p < z, arrived[p, 16:24, :], 0.0)
    counts_out[...] = counts


def start_kernel(far, arrived, counts, out, closing):
    parts = []
    for p in range(RING):
        parts.append(far[p, 0:16, :])
        closing[16 * p : 16 * p + 16, :] = far[p, 16:32, :]
    acc = jnp.concatenate(parts + [counts[...]], axis=0)
    for k in range(SIB):
        i = 2 * (k % 4) + k // 4
        out[i] = acc
        acc = acc + arrived[i]


def running_kernel(start, local, slot, cols, closed, mean, count, closing, left, held_mean, sems):
    sub = lax.broadcasted_iota(jnp.int32, (16, LANES), 0)
    for j in range(NT):
        for h in range(2):
            a, b, _ = pieces(start[j, h * 64 : (h + 1) * 64, :])
            n = pieces(start[j, 128 + h : 129 + h, :])
            n = [jnp.broadcast_to(v.astype(F32), (16, LANES)) for v in n]
            n = jnp.where(sub == 0, n[0], jnp.where(sub == 1, n[1], jnp.where(sub == 2, n[2], 0.0)))
            top = (j // NH) * LHS
            at = (j % NH) * T + h * LANES
            left[top : top + LHS, at : at + LANES] = jnp.concatenate([a, b, n.astype(BF16)], axis=0)
    label = lax.broadcasted_iota(jnp.int32, (T, T), 0)
    order = label <= lax.broadcasted_iota(jnp.int32, (T, T), 1)
    copies = []
    for j in range(NT):
        row = jnp.concatenate([slot[2 * j : 2 * j + 1, :], slot[2 * j + 1 : 2 * j + 2, :]], axis=1)
        high = jnp.broadcast_to(row, (LHS, T)) >= HALF
        row = jnp.broadcast_to(row, (T, T))
        low = jnp.bitwise_and(row, HALF - 1)
        res = None
        for k in range(NH):
            part = dot(left[:, k * T : (k + 1) * T], hot(label + k * T == low))
            res = part if res is None else res + part
        own = None
        for k in range(j + 1):
            at = slice(k * T, (k + 1) * T)
            keys = cols[at, :]
            mask = jnp.concatenate([keys, keys], axis=1) == row
            if k == j:
                mask = jnp.logical_and(mask, order)
            part = dot(local[:, at], hot(mask))
            own = part if own is None else own + part
        res = jnp.where(high, res[LHS : 2 * LHS], res[0:LHS]) + own
        total = res[0:64] + res[64:128]
        tally = (res[128:129] + res[129:130]) + res[130:131]
        at = slice(j * T, (j + 1) * T)
        held_mean[:, at] = total / tally
        copies.append(pltpu.make_async_copy(held_mean.at[:, at], mean.at[:, at], sems.at[j]))
        copies[-1].start()
        whole = tally.astype(jnp.int32)
        count[2 * j : 2 * j + 1, :] = whole[:, :LANES]
        count[2 * j + 1 : 2 * j + 2, :] = whole[:, LANES:]
    for c in range(2):
        for h in range(2):
            closing[:, c * T + h * LANES : c * T + (h + 1) * LANES] = closed[c, h * 64 : (h + 1) * 64, :]
    for copy in copies:
        copy.wait()


def shape(*dims, dtype=F32):
    return jax.ShapeDtypeStruct(dims, dtype)


def near(*dims, dtype=F32):
    return pltpu.VMEM(dims, dtype)


def outer(x):
    return pltpu.with_memory_space_constraint(x, pltpu.HBM)


def held(x):
    return pltpu.with_memory_space_constraint(x, pltpu.VMEM)


def sums_call(vt, gid, table):
    outside = pl.BlockSpec(memory_space=pl.ANY)
    return pl.pallas_call(
        sums_kernel,
        in_specs=[outside] * 3,
        out_shape=(
            near(SIB, MSG, LANES),
            near(16, LANES, dtype=jnp.int32),
            near(LHS, R, dtype=BF16),
            near(R, LANES, dtype=jnp.int32),
        ),
        scratch_shapes=[
            pltpu.VMEM((M, R), F32),
            pltpu.VMEM((16, LANES), jnp.int32),
            pltpu.VMEM((16, LANES), jnp.int32),
            pltpu.VMEM((2 * LHS, R), BF16),
            pltpu.SemaphoreType.DMA((7,)),
        ],
        compiler_params=ROOM,
        name="local_sums",
    )(outer(vt), outer(gid), outer(table))


def running_call(start, local, slot, cols, closed):
    vmem = pl.BlockSpec(memory_space=pltpu.VMEM)
    return pl.pallas_call(
        running_kernel,
        out_shape=(shape(M, R), shape(16, LANES, dtype=jnp.int32), shape(M, 512)),
        out_specs=(pl.BlockSpec(memory_space=pl.ANY), vmem, vmem),
        scratch_shapes=[
            pltpu.VMEM((2 * LHS, HALF), BF16),
            pltpu.VMEM((M, R), F32),
            pltpu.SemaphoreType.DMA((NT,)),
        ],
        compiler_params=ROOM,
        name="running_means",
    )(start, held(local), held(slot), held(cols), closed)


def local(values, group_ids, slot_of):
    vt = values.T
    gid = group_ids.reshape(16, LANES)
    table = slot_of.reshape(16, LANES)
    sums, slot, local_pieces, cols = sums_call(vt, gid, table)
    siblings = ("x", "c")
    arrived = held(lax.all_to_all(sums, siblings, 0, 0, tiled=True))
    parts = pl.pallas_call(
        slice_kernel,
        out_shape=near(RING, 24, LANES),
        compiler_params=ROOM,
        name="slice_sums",
    )(arrived)
    along_z = held(lax.all_to_all(parts, "z", 0, 0, tiled=True))
    ring = pl.pallas_call(
        ring_kernel,
        out_shape=near(RING, 24, LANES),
        compiler_params=ROOM,
        name="ring_sums",
    )(along_z)
    along_y = held(lax.all_to_all(ring, "y", 0, 0, tiled=True))
    scanned, counts = pl.pallas_call(
        scan_kernel,
        out_shape=(near(RING, 32, LANES), near(8, LANES)),
        compiler_params=ROOM,
        name="scan",
    )(along_z, along_y)
    back = held(lax.all_to_all(scanned, "z", 0, 0, tiled=True))
    starts, closing_half = pl.pallas_call(
        start_kernel,
        out_shape=(near(SIB, MSG, LANES), near(LANES, LANES)),
        compiler_params=ROOM,
        name="starts",
    )(back, arrived, counts)
    closed = lax.all_gather(closing_half, "c")
    starts, closed = lax.optimization_barrier((starts, closed))
    closed = held(closed)
    start = held(lax.all_to_all(starts, siblings, 0, 0, tiled=True))
    mean, count, closing = running_call(start, local_pieces, slot, cols, closed)
    return mean.T, count.reshape(R), closing.T


def solution(mesh):
    split = Mesh(mesh.devices.reshape(8, 8, 2, 4), ROWS_ALL)
    in_specs = (P(ROWS_ALL, None), P(ROWS_ALL), P())
    out_specs = (P(ROWS_ALL, None), P(ROWS_ALL), P("x", None))
    return jax.shard_map(local, mesh=split, in_specs=in_specs, out_specs=out_specs, check_vma=False)
```

```python
import jax
import jax.numpy as jnp
from jax import lax
from jax.experimental import pallas as pl
from jax.experimental.pallas import tpu as pltpu
from jax.sharding import Mesh
from jax.sharding import PartitionSpec as P

ROWS_ALL = ("y", "z", "c", "x")
F32 = jnp.float32
BF16 = jnp.bfloat16
M = 64
R = 2048
S = 2048
LANES = 128
T = 256
NT = S // T
NH = NT // 2
SIB = 8
RING = 8
MSG = 136
LHS = 144
HALF = 1024


ROOM = pltpu.CompilerParams(vmem_limit_bytes=16 << 20)


def pieces(v):
    a = v.astype(BF16)
    rest = v - a.astype(F32)
    b = rest.astype(BF16)
    c = (rest - b.astype(F32)).astype(BF16)
    return a, b, c


def lookup(table, idx):
    low = jnp.bitwise_and(idx, LANES - 1)
    high = jnp.right_shift(idx, 7)
    out = jnp.zeros_like(idx)
    for k in range(S // LANES):
        row = jnp.broadcast_to(table[k : k + 1, :], idx.shape)
        out = jnp.where(high == k, jnp.take_along_axis(row, low, axis=1), out)
    return out


def columns(slot):
    flipped = jnp.concatenate([slot] * 8, axis=0).T
    return [jnp.broadcast_to(flipped[:, i : i + 1], (LANES, LANES)) for i in range(R // LANES)]


def dot(a, b):
    return lax.dot_general(a, b, (((1,), (0,)), ((), ())), preferred_element_type=F32)


def hot(mask):
    return jnp.where(mask, 1.0, 0.0).astype(BF16)


def sums_kernel(vt_far, gid_far, table_far, out, slot_out, local, cols, vt, gid, table, split, sems):
    values_in = [
        pltpu.make_async_copy(vt_far.at[16 * g : 16 * g + 16], vt.at[16 * g : 16 * g + 16], sems.at[3 + g]) for g in range(4)
    ]
    keys_in = pltpu.make_async_copy(gid_far, gid, sems.at[1])
    table_in = pltpu.make_async_copy(table_far, table, sems.at[2])
    keys_in.start()
    table_in.start()
    for copy in values_in:
        copy.start()
    keys_in.wait()
    table_in.wait()
    slot = lookup(table[...], gid[...])
    slot_out[...] = slot
    sub = lax.broadcasted_iota(jnp.int32, (16, LANES), 0)
    ones = jnp.where(sub == 0, 1.0, 0.0)
    spans = [slice(i * LANES, (i + 1) * LANES) for i in range(R // LANES)]
    highs = [jnp.broadcast_to(slot[i : i + 1, :], (16, LANES)) >= HALF for i in range(R // LANES)]

    def place(rows, value):
        for at, high in zip(spans, highs):
            v = value[:, at] if value.shape[1] > LANES else value
            local[rows : rows + 16, at] = v.astype(BF16)
            split[rows : rows + 16, at] = jnp.where(high, 0.0, v).astype(BF16)
            split[LHS + rows : LHS + rows + 16, at] = jnp.where(high, v, 0.0).astype(BF16)

    place(128, ones)
    for g in range(4):
        values_in[g].wait()
        a, b, _ = pieces(vt[16 * g : 16 * g + 16, :])
        place(16 * g, a.astype(F32))
        place(64 + 16 * g, b.astype(F32))
    for i, block in enumerate(columns(slot)):
        cols[i * LANES : (i + 1) * LANES, :] = block
    lane = lax.broadcasted_iota(jnp.int32, (T, T), 1)
    first = lax.broadcasted_iota(jnp.int32, (8, LANES), 0) == 0
    for j in range(NH):
        res = None
        for k in range(NT):
            at = slice(k * T, (k + 1) * T)
            keys = jnp.bitwise_and(cols[at, :], HALF - 1)
            keys = jnp.concatenate([keys, keys], axis=1)
            part = dot(split[:, at], hot(keys == lane + j * T))
            res = part if res is None else res + part
        for h in range(2):
            of = res[h * LHS : (h + 1) * LHS]
            total = of[0:64] + of[64:128]
            to = h * NH + j
            out[to, 0:64, :] = total[:, :LANES]
            out[to, 64:128, :] = total[:, LANES:]
            number = jnp.broadcast_to(of[128:129], (8, T))
            out[to, 128:136, :] = jnp.where(first, number[:, :LANES], number[:, LANES:])


def slice_kernel(arrived, out):
    total = arrived[0]
    for i in range(1, SIB):
        total = total + arrived[i]
    for p in range(RING):
        out[p, 0:16, :] = total[16 * p : 16 * p + 16]
        out[p, 16:24, :] = total[128:136]


def ring_kernel(arrived, out):
    total = arrived[0]
    for i in range(1, RING):
        total = total + arrived[i]
    for p in range(RING):
        out[p] = total


def scan_kernel(arrived, rings, out, counts_out):
    y = lax.axis_index("y")
    z = lax.axis_index("z")
    total = rings[0]
    before = jnp.where(y > 0, total, 0.0)
    for i in range(1, RING):
        ring = rings[i]
        before = before + jnp.where(i < y, ring, 0.0)
        total = total + ring
    number = jnp.where(z < RING // 2, total[16:17], total[17:18])
    closing = total[0:16] / jnp.maximum(number, 1.0)
    counts = before[16:24]
    acc = before[0:16]
    for p in range(RING):
        out[p, 0:16, :] = acc
        out[p, 16:32, :] = closing
        acc = acc + arrived[p, 0:16, :]
        counts = counts + jnp.where(p < z, arrived[p, 16:24, :], 0.0)
    counts_out[...] = counts


def start_kernel(far, arrived, counts, out, closing):
    parts = []
    for p in range(RING):
        parts.append(far[p, 0:16, :])
        closing[16 * p : 16 * p + 16, :] = far[p, 16:32, :]
    acc = jnp.concatenate(parts + [counts[...]], axis=0)
    for k in range(SIB):
        i = 2 * (k % 4) + k // 4
        out[i] = acc
        acc = acc + arrived[i]


def both(slot, j):
    return jnp.concatenate([slot[2 * j : 2 * j + 1, :], slot[2 * j + 1 : 2 * j + 2, :]], axis=1)


def own_kernel(local, slot, cols, out):
    label = lax.broadcasted_iota(jnp.int32, (T, T), 0)
    order = label <= lax.broadcasted_iota(jnp.int32, (T, T), 1)
    for j in range(NT):
        row = jnp.broadcast_to(both(slot, j), (T, T))
        own = None
        for k in range(j + 1):
            at = slice(k * T, (k + 1) * T)
            keys = cols[at, :]
            mask = jnp.concatenate([keys, keys], axis=1) == row
            if k == j:
                mask = jnp.logical_and(mask, order)
            part = dot(local[:, at], hot(mask))
            own = part if own is None else own + part
        at = slice(j * T, (j + 1) * T)
        out[0:64, at] = own[0:64] + own[64:128]
        out[64:72, at] = own[128:136]


def running_kernel(start, own, slot, closed, mean, count, closing, left, held_mean, sems):
    sub = lax.broadcasted_iota(jnp.int32, (16, LANES), 0)
    for j in range(NT):
        for h in range(2):
            a, b, _ = pieces(start[j, h * 64 : (h + 1) * 64, :])
            n = pieces(start[j, 128 + h : 129 + h, :])
            n = [jnp.broadcast_to(v.astype(F32), (16, LANES)) for v in n]
            n = jnp.where(sub == 0, n[0], jnp.where(sub == 1, n[1], jnp.where(sub == 2, n[2], 0.0)))
            top = (j // NH) * LHS
            at = (j % NH) * T + h * LANES
            left[top : top + LHS, at : at + LANES] = jnp.concatenate([a, b, n.astype(BF16)], axis=0)
    label = lax.broadcasted_iota(jnp.int32, (T, T), 0)
    copies = []
    for j in range(NT):
        row = both(slot, j)
        high = jnp.broadcast_to(row, (LHS, T)) >= HALF
        low = jnp.bitwise_and(jnp.broadcast_to(row, (T, T)), HALF - 1)
        res = None
        for k in range(NH):
            part = dot(left[:, k * T : (k + 1) * T], hot(label + k * T == low))
            res = part if res is None else res + part
        res = jnp.where(high, res[LHS : 2 * LHS], res[0:LHS])
        at = slice(j * T, (j + 1) * T)
        total = res[0:64] + res[64:128] + own[0:64, at]
        tally = (res[128:129] + res[129:130]) + res[130:131] + own[64:65, at]
        held_mean[:, at] = total / tally
        copies.append(pltpu.make_async_copy(held_mean.at[:, at], mean.at[:, at], sems.at[j]))
        copies[-1].start()
        whole = tally.astype(jnp.int32)
        count[2 * j : 2 * j + 1, :] = whole[:, :LANES]
        count[2 * j + 1 : 2 * j + 2, :] = whole[:, LANES:]
    for c in range(2):
        for h in range(2):
            closing[:, c * T + h * LANES : c * T + (h + 1) * LANES] = closed[c, h * 64 : (h + 1) * 64, :]
    for copy in copies:
        copy.wait()


def shape(*dims, dtype=F32):
    return jax.ShapeDtypeStruct(dims, dtype)


def near(*dims, dtype=F32):
    return pltpu.VMEM(dims, dtype)


def outer(x):
    return pltpu.with_memory_space_constraint(x, pltpu.HBM)


def held(x):
    return pltpu.with_memory_space_constraint(x, pltpu.VMEM)


def sums_call(vt, gid, table):
    outside = pl.BlockSpec(memory_space=pl.ANY)
    return pl.pallas_call(
        sums_kernel,
        in_specs=[outside] * 3,
        out_shape=(
            near(SIB, MSG, LANES),
            near(16, LANES, dtype=jnp.int32),
            near(LHS, R, dtype=BF16),
            near(R, LANES, dtype=jnp.int32),
        ),
        scratch_shapes=[
            pltpu.VMEM((M, R), F32),
            pltpu.VMEM((16, LANES), jnp.int32),
            pltpu.VMEM((16, LANES), jnp.int32),
            pltpu.VMEM((2 * LHS, R), BF16),
            pltpu.SemaphoreType.DMA((7,)),
        ],
        compiler_params=ROOM,
        name="local_sums",
    )(outer(vt), outer(gid), outer(table))


def own_call(local, slot, cols):
    return pl.pallas_call(
        own_kernel,
        out_shape=near(72, R),
        compiler_params=ROOM,
        cost_estimate=pl.CostEstimate(flops=2 * 144 * R * R // 2, bytes_accessed=1 << 20, transcendentals=0),
        name="own_rows",
    )(held(local), held(slot), held(cols))


def running_call(start, own, slot, closed):
    vmem = pl.BlockSpec(memory_space=pltpu.VMEM)
    return pl.pallas_call(
        running_kernel,
        out_shape=(shape(M, R), shape(16, LANES, dtype=jnp.int32), shape(M, 512)),
        out_specs=(pl.BlockSpec(memory_space=pl.ANY), vmem, vmem),
        scratch_shapes=[
            pltpu.VMEM((2 * LHS, HALF), BF16),
            pltpu.VMEM((M, R), F32),
            pltpu.SemaphoreType.DMA((NT,)),
        ],
        compiler_params=ROOM,
        name="running_means",
    )(start, held(own), held(slot), closed)


def local(values, group_ids, slot_of):
    vt = values.T
    gid = group_ids.reshape(16, LANES)
    table = slot_of.reshape(16, LANES)
    sums, slot, local_pieces, cols = sums_call(vt, gid, table)
    siblings = ("x", "c")
    arrived = held(lax.all_to_all(sums, siblings, 0, 0, tiled=True))
    parts = pl.pallas_call(
        slice_kernel,
        out_shape=near(RING, 24, LANES),
        compiler_params=ROOM,
        name="slice_sums",
    )(arrived)
    along_z = held(lax.all_to_all(parts, "z", 0, 0, tiled=True))
    ring = pl.pallas_call(
        ring_kernel,
        out_shape=near(RING, 24, LANES),
        compiler_params=ROOM,
        name="ring_sums",
    )(along_z)
    along_y = held(lax.all_to_all(ring, "y", 0, 0, tiled=True))
    scanned, counts = pl.pallas_call(
        scan_kernel,
        out_shape=(near(RING, 32, LANES), near(8, LANES)),
        compiler_params=ROOM,
        name="scan",
    )(along_z, along_y)
    back = held(lax.all_to_all(scanned, "z", 0, 0, tiled=True))
    starts, closing_half = pl.pallas_call(
        start_kernel,
        out_shape=(near(SIB, MSG, LANES), near(LANES, LANES)),
        compiler_params=ROOM,
        name="starts",
    )(back, arrived, counts)
    closed = held(lax.all_gather(closing_half, "c"))
    own = own_call(local_pieces, slot, cols)
    start = held(lax.all_to_all(starts, siblings, 0, 0, tiled=True))
    mean, count, closing = running_call(start, own, slot, closed)
    return mean.T, count.reshape(R), closing.T


def solution(mesh):
    split = Mesh(mesh.devices.reshape(8, 8, 2, 4), ROWS_ALL)
    in_specs = (P(ROWS_ALL, None), P(ROWS_ALL), P())
    out_specs = (P(ROWS_ALL, None), P(ROWS_ALL), P("x", None))
    return jax.shard_map(local, mesh=split, in_specs=in_specs, out_specs=out_specs, check_vma=False)
```

```python
import jax
import jax.numpy as jnp
from jax import lax
from jax.experimental import pallas as pl
from jax.experimental.pallas import tpu as pltpu
from jax.sharding import Mesh
from jax.sharding import PartitionSpec as P

ROWS_ALL = ("y", "z", "c", "x")
F32 = jnp.float32
BF16 = jnp.bfloat16
M = 64
R = 2048
S = 2048
LANES = 128
T = 256
NT = S // T
NH = NT // 2
SIB = 8
RING = 8
MSG = 136
LHS = 144
HALF = 1024


ROOM = pltpu.CompilerParams(vmem_limit_bytes=16 << 20)


def pieces(v):
    a = v.astype(BF16)
    rest = v - a.astype(F32)
    b = rest.astype(BF16)
    c = (rest - b.astype(F32)).astype(BF16)
    return a, b, c


def lookup(table, idx):
    low = jnp.bitwise_and(idx, LANES - 1)
    high = jnp.right_shift(idx, 7)
    out = jnp.zeros_like(idx)
    for k in range(S // LANES):
        row = jnp.broadcast_to(table[k : k + 1, :], idx.shape)
        out = jnp.where(high == k, jnp.take_along_axis(row, low, axis=1), out)
    return out


def columns(slot):
    flipped = jnp.concatenate([slot] * 8, axis=0).T
    return [jnp.broadcast_to(flipped[:, i : i + 1], (LANES, LANES)) for i in range(R // LANES)]


def dot(a, b):
    return lax.dot_general(a, b, (((1,), (0,)), ((), ())), preferred_element_type=F32)


def hot(mask):
    return jnp.where(mask, 1.0, 0.0).astype(BF16)


def sums_kernel(vt_far, gid_far, table_far, out, slot_out, split, cols, vt, gid, table, sems):
    values_in = [
        pltpu.make_async_copy(vt_far.at[16 * g : 16 * g + 16], vt.at[16 * g : 16 * g + 16], sems.at[3 + g]) for g in range(4)
    ]
    keys_in = pltpu.make_async_copy(gid_far, gid, sems.at[1])
    table_in = pltpu.make_async_copy(table_far, table, sems.at[2])
    keys_in.start()
    table_in.start()
    for copy in values_in:
        copy.start()
    keys_in.wait()
    table_in.wait()
    slot = lookup(table[...], gid[...])
    slot_out[...] = slot
    sub = lax.broadcasted_iota(jnp.int32, (16, LANES), 0)
    ones = jnp.where(sub == 0, 1.0, 0.0).astype(BF16)
    spans = [slice(i * LANES, (i + 1) * LANES) for i in range(R // LANES)]
    high = jnp.where(slot >= HALF, 1.0, 0.0)
    highs = [jnp.broadcast_to(high[i : i + 1, :], (16, LANES)) for i in range(R // LANES)]
    picks = [((1.0 - h).astype(BF16), h.astype(BF16)) for h in highs]

    def place(rows, at, value, pick):
        split[rows : rows + 16, at] = value * pick[0]
        split[LHS + rows : LHS + rows + 16, at] = value * pick[1]

    for at, pick in zip(spans, picks):
        place(128, at, ones, pick)
    for g in range(4):
        values_in[g].wait()
        for at, pick in zip(spans, picks):
            a, b, _ = pieces(vt[16 * g : 16 * g + 16, at])
            place(16 * g, at, a, pick)
            place(64 + 16 * g, at, b, pick)
    for i, block in enumerate(columns(slot)):
        cols[i * LANES : (i + 1) * LANES, :] = block
    lane = lax.broadcasted_iota(jnp.int32, (T, T), 1)
    first = lax.broadcasted_iota(jnp.int32, (8, LANES), 0) == 0
    for j in range(NH):
        res = None
        for k in range(NT):
            at = slice(k * T, (k + 1) * T)
            keys = jnp.bitwise_and(cols[at, :], HALF - 1)
            keys = jnp.concatenate([keys, keys], axis=1)
            part = dot(split[:, at], hot(keys == lane + j * T))
            res = part if res is None else res + part
        for h in range(2):
            of = res[h * LHS : (h + 1) * LHS]
            total = of[0:64] + of[64:128]
            to = h * NH + j
            out[to, 0:64, :] = total[:, :LANES]
            out[to, 64:128, :] = total[:, LANES:]
            number = jnp.broadcast_to(of[128:129], (8, T))
            out[to, 128:136, :] = jnp.where(first, number[:, :LANES], number[:, LANES:])


def slice_kernel(arrived, out):
    total = arrived[0]
    for i in range(1, SIB):
        total = total + arrived[i]
    for p in range(RING):
        out[p, 0:16, :] = total[16 * p : 16 * p + 16]
        out[p, 16:24, :] = total[128:136]


def ring_kernel(arrived, out):
    total = arrived[0]
    for i in range(1, RING):
        total = total + arrived[i]
    for p in range(RING):
        out[p] = total


def scan_kernel(arrived, rings, out, counts_out):
    y = lax.axis_index("y")
    z = lax.axis_index("z")
    total = rings[0]
    before = jnp.where(y > 0, total, 0.0)
    for i in range(1, RING):
        ring = rings[i]
        before = before + jnp.where(i < y, ring, 0.0)
        total = total + ring
    number = jnp.where(z < RING // 2, total[16:17], total[17:18])
    closing = total[0:16] / jnp.maximum(number, 1.0)
    counts = before[16:24]
    acc = before[0:16]
    for p in range(RING):
        out[p, 0:16, :] = acc
        out[p, 16:32, :] = closing
        acc = acc + arrived[p, 0:16, :]
        counts = counts + jnp.where(p < z, arrived[p, 16:24, :], 0.0)
    counts_out[...] = counts


def start_kernel(far, arrived, counts, out_far, closing, out, sems):
    parts = []
    for p in range(RING):
        parts.append(far[p, 0:16, :])
        closing[16 * p : 16 * p + 16, :] = far[p, 16:32, :]
    acc = jnp.concatenate(parts + [counts[...]], axis=0)
    copies = []
    for k in range(SIB):
        i = 2 * (k % 4) + k // 4
        out[i] = acc
        copies.append(pltpu.make_async_copy(out.at[i], out_far.at[i], sems.at[i]))
        copies[-1].start()
        acc = acc + arrived[i]
    for copy in copies:
        copy.wait()


def both(slot, j):
    return jnp.concatenate([slot[2 * j : 2 * j + 1, :], slot[2 * j + 1 : 2 * j + 2, :]], axis=1)


def own_kernel(split, slot, cols, out, local):
    local[...] = split[0:LHS, :] + split[LHS : 2 * LHS, :]
    label = lax.broadcasted_iota(jnp.int32, (T, T), 0)
    order = label <= lax.broadcasted_iota(jnp.int32, (T, T), 1)
    for j in range(NT):
        row = jnp.broadcast_to(both(slot, j), (T, T))
        own = None
        for k in range(j + 1):
            at = slice(k * T, (k + 1) * T)
            keys = cols[at, :]
            mask = jnp.concatenate([keys, keys], axis=1) == row
            if k == j:
                mask = jnp.logical_and(mask, order)
            part = dot(local[:, at], hot(mask))
            own = part if own is None else own + part
        at = slice(j * T, (j + 1) * T)
        out[0:64, at] = own[0:64] + own[64:128]
        out[64:72, at] = own[128:136]


def running_kernel(start, own, slot, closed, mean, count_far, closing_far, left, held_mean, count, closing, sems):
    for c in range(2):
        for h in range(2):
            closing[:, c * T + h * LANES : c * T + (h + 1) * LANES] = closed[c, h * 64 : (h + 1) * 64, :]
    copies = [pltpu.make_async_copy(closing, closing_far, sems.at[NT])]
    copies[0].start()
    sub = lax.broadcasted_iota(jnp.int32, (16, LANES), 0)
    for j in range(NT):
        for h in range(2):
            a, b, _ = pieces(start[j, h * 64 : (h + 1) * 64, :])
            n = pieces(start[j, 128 + h : 129 + h, :])
            n = [jnp.broadcast_to(v.astype(F32), (16, LANES)) for v in n]
            n = jnp.where(sub == 0, n[0], jnp.where(sub == 1, n[1], jnp.where(sub == 2, n[2], 0.0)))
            top = (j // NH) * LHS
            at = (j % NH) * T + h * LANES
            left[top : top + LHS, at : at + LANES] = jnp.concatenate([a, b, n.astype(BF16)], axis=0)
    label = lax.broadcasted_iota(jnp.int32, (T, T), 0)
    for j in range(NT):
        row = both(slot, j)
        high = jnp.broadcast_to(row, (LHS, T)) >= HALF
        low = jnp.bitwise_and(jnp.broadcast_to(row, (T, T)), HALF - 1)
        res = None
        for k in range(NH):
            part = dot(left[:, k * T : (k + 1) * T], hot(label + k * T == low))
            res = part if res is None else res + part
        res = jnp.where(high, res[LHS : 2 * LHS], res[0:LHS])
        at = slice(j * T, (j + 1) * T)
        total = res[0:64] + res[64:128] + own[0:64, at]
        tally = (res[128:129] + res[129:130]) + res[130:131] + own[64:65, at]
        held_mean[:, at] = total / tally
        copies.append(pltpu.make_async_copy(held_mean.at[:, at], mean.at[:, at], sems.at[j]))
        copies[-1].start()
        whole = tally.astype(jnp.int32)
        count[2 * j : 2 * j + 1, :] = whole[:, :LANES]
        count[2 * j + 1 : 2 * j + 2, :] = whole[:, LANES:]
    copies.append(pltpu.make_async_copy(count, count_far, sems.at[NT + 1]))
    copies[-1].start()
    for copy in copies:
        copy.wait()


def shape(*dims, dtype=F32):
    return jax.ShapeDtypeStruct(dims, dtype)


def near(*dims, dtype=F32):
    return pltpu.VMEM(dims, dtype)


def outward(*dims):
    return pltpu.HBM(dims, F32)


def outer(x):
    return pltpu.with_memory_space_constraint(x, pltpu.HBM)


def held(x):
    return pltpu.with_memory_space_constraint(x, pltpu.VMEM)


def sums_call(vt, gid, table):
    outside = pl.BlockSpec(memory_space=pl.ANY)
    return pl.pallas_call(
        sums_kernel,
        in_specs=[outside] * 3,
        out_shape=(
            near(SIB, MSG, LANES),
            near(16, LANES, dtype=jnp.int32),
            near(2 * LHS, R, dtype=BF16),
            near(R, LANES, dtype=jnp.int32),
        ),
        scratch_shapes=[
            pltpu.VMEM((M, R), F32),
            pltpu.VMEM((16, LANES), jnp.int32),
            pltpu.VMEM((16, LANES), jnp.int32),
            pltpu.SemaphoreType.DMA((7,)),
        ],
        compiler_params=ROOM,
        name="local_sums",
    )(outer(vt), outer(gid), outer(table))


def own_call(split, slot, cols):
    return pl.pallas_call(
        own_kernel,
        out_shape=near(72, R),
        scratch_shapes=[pltpu.VMEM((LHS, R), BF16)],
        compiler_params=ROOM,
        cost_estimate=pl.CostEstimate(flops=2 * 144 * R * R // 2, bytes_accessed=1 << 20, transcendentals=0),
        name="own_rows",
    )(held(split), held(slot), held(cols))


def running_call(start, own, slot, closed):
    return pl.pallas_call(
        running_kernel,
        out_shape=(shape(M, R), shape(16, LANES, dtype=jnp.int32), shape(M, 512)),
        out_specs=(pl.BlockSpec(memory_space=pl.ANY),) * 3,
        scratch_shapes=[
            pltpu.VMEM((2 * LHS, HALF), BF16),
            pltpu.VMEM((M, R), F32),
            pltpu.VMEM((16, LANES), jnp.int32),
            pltpu.VMEM((M, 2 * T), F32),
            pltpu.SemaphoreType.DMA((NT + 2,)),
        ],
        compiler_params=ROOM,
        name="running_means",
    )(start, held(own), held(slot), closed)


def local(values, group_ids, slot_of):
    vt = values.T
    gid = group_ids.reshape(16, LANES)
    table = slot_of.reshape(16, LANES)
    sums, slot, split, cols = sums_call(vt, gid, table)
    siblings = ("x", "c")
    arrived = held(lax.all_to_all(sums, siblings, 0, 0, tiled=True))
    parts = pl.pallas_call(
        slice_kernel,
        out_shape=near(RING, 24, LANES),
        compiler_params=ROOM,
        name="slice_sums",
    )(arrived)
    along_z = held(lax.all_to_all(parts, "z", 0, 0, tiled=True))
    ring = pl.pallas_call(
        ring_kernel,
        out_shape=near(RING, 24, LANES),
        compiler_params=ROOM,
        name="ring_sums",
    )(along_z)
    along_y = held(lax.all_to_all(ring, "y", 0, 0, tiled=True))
    scanned, counts = pl.pallas_call(
        scan_kernel,
        out_shape=(near(RING, 32, LANES), near(8, LANES)),
        compiler_params=ROOM,
        name="scan",
    )(along_z, along_y)
    back = held(lax.all_to_all(scanned, "z", 0, 0, tiled=True))
    starts, closing_half = pl.pallas_call(
        start_kernel,
        out_shape=(outward(SIB, MSG, LANES), near(LANES, LANES)),
        out_specs=(pl.BlockSpec(memory_space=pl.ANY), pl.BlockSpec(memory_space=pltpu.VMEM)),
        scratch_shapes=[pltpu.VMEM((SIB, MSG, LANES), F32), pltpu.SemaphoreType.DMA((SIB,))],
        compiler_params=ROOM,
        name="starts",
    )(back, arrived, counts)
    closed = held(lax.all_gather(closing_half, "c"))
    own = own_call(split, slot, cols)
    start = held(lax.all_to_all(starts, siblings, 0, 0, tiled=True))
    mean, count, closing = running_call(start, own, slot, closed)
    return mean.T, count.reshape(R), closing.T


def solution(mesh):
    split = Mesh(mesh.devices.reshape(8, 8, 2, 4), ROWS_ALL)
    in_specs = (P(ROWS_ALL, None), P(ROWS_ALL), P())
    out_specs = (P(ROWS_ALL, None), P(ROWS_ALL), P("x", None))
    return jax.shard_map(local, mesh=split, in_specs=in_specs, out_specs=out_specs, check_vma=False)
```

```python
import jax
import jax.numpy as jnp
from jax import lax
from jax.experimental import pallas as pl
from jax.experimental.pallas import tpu as pltpu
from jax.sharding import Mesh
from jax.sharding import PartitionSpec as P

ROWS_ALL = ("y", "z", "c", "x")
F32 = jnp.float32
BF16 = jnp.bfloat16
M = 64
R = 2048
S = 2048
LANES = 128
T = 256
NT = S // T
NH = NT // 2
SIB = 8
FAR = 64
MSG = 136
LHS = 144
HALF = 1024


ROOM = pltpu.CompilerParams(vmem_limit_bytes=16 << 20)


def pieces(v):
    a = v.astype(BF16)
    rest = v - a.astype(F32)
    b = rest.astype(BF16)
    c = (rest - b.astype(F32)).astype(BF16)
    return a, b, c


def lookup(table, idx):
    low = jnp.bitwise_and(idx, LANES - 1)
    high = jnp.right_shift(idx, 7)
    out = jnp.zeros_like(idx)
    for k in range(S // LANES):
        row = jnp.broadcast_to(table[k : k + 1, :], idx.shape)
        out = jnp.where(high == k, jnp.take_along_axis(row, low, axis=1), out)
    return out


def columns(slot):
    flipped = jnp.concatenate([slot] * 8, axis=0).T
    return [jnp.broadcast_to(flipped[:, i : i + 1], (LANES, LANES)) for i in range(R // LANES)]


def dot(a, b):
    return lax.dot_general(a, b, (((1,), (0,)), ((), ())), preferred_element_type=F32)


def hot(mask):
    return jnp.where(mask, 1.0, 0.0).astype(BF16)


def sums_kernel(vt_far, gid_far, table_far, out, slot_out, split, cols, vt, gid, table, sems):
    values_in = [
        pltpu.make_async_copy(vt_far.at[16 * g : 16 * g + 16], vt.at[16 * g : 16 * g + 16], sems.at[3 + g]) for g in range(4)
    ]
    keys_in = pltpu.make_async_copy(gid_far, gid, sems.at[1])
    table_in = pltpu.make_async_copy(table_far, table, sems.at[2])
    keys_in.start()
    table_in.start()
    for copy in values_in:
        copy.start()
    keys_in.wait()
    table_in.wait()
    slot = lookup(table[...], gid[...])
    slot_out[...] = slot
    sub = lax.broadcasted_iota(jnp.int32, (16, LANES), 0)
    ones = jnp.where(sub == 0, 1.0, 0.0).astype(BF16)
    spans = [slice(i * LANES, (i + 1) * LANES) for i in range(R // LANES)]
    high = jnp.where(slot >= HALF, 1.0, 0.0)
    highs = [jnp.broadcast_to(high[i : i + 1, :], (16, LANES)) for i in range(R // LANES)]
    picks = [((1.0 - h).astype(BF16), h.astype(BF16)) for h in highs]

    def place(rows, at, value, pick):
        split[rows : rows + 16, at] = value * pick[0]
        split[LHS + rows : LHS + rows + 16, at] = value * pick[1]

    for at, pick in zip(spans, picks):
        place(128, at, ones, pick)
    for g in range(4):
        values_in[g].wait()
        for at, pick in zip(spans, picks):
            a, b, _ = pieces(vt[16 * g : 16 * g + 16, at])
            place(16 * g, at, a, pick)
            place(64 + 16 * g, at, b, pick)
    for i, block in enumerate(columns(slot)):
        cols[i * LANES : (i + 1) * LANES, :] = block
    lane = lax.broadcasted_iota(jnp.int32, (T, T), 1)
    first = lax.broadcasted_iota(jnp.int32, (8, LANES), 0) == 0
    for j in range(NH):
        res = None
        for k in range(NT):
            at = slice(k * T, (k + 1) * T)
            keys = jnp.bitwise_and(cols[at, :], HALF - 1)
            keys = jnp.concatenate([keys, keys], axis=1)
            part = dot(split[:, at], hot(keys == lane + j * T))
            res = part if res is None else res + part
        for h in range(2):
            of = res[h * LHS : (h + 1) * LHS]
            total = of[0:64] + of[64:128]
            to = h * NH + j
            out[to, 0:64, :] = total[:, :LANES]
            out[to, 64:128, :] = total[:, LANES:]
            number = jnp.broadcast_to(of[128:129], (8, T))
            out[to, 128:136, :] = jnp.where(first, number[:, :LANES], number[:, LANES:])


def slice_kernel(arrived, out, buf):
    total = arrived[0]
    for i in range(1, SIB):
        total = total + arrived[i]
    buf[...] = total
    counts = buf[128:130, :]
    for p in range(FAR):
        out[p, 0:2, :] = buf[2 * p : 2 * p + 2, :]
        out[p, 2:4, :] = counts


def scan_kernel(arrived, out, counts_out):
    mine = lax.axis_index("y") * 8 + lax.axis_index("z")
    acc = jnp.zeros((4, LANES), F32)
    before = jnp.zeros((4, LANES), F32)
    for p in range(FAR):
        got = arrived[p]
        out[p, 0:2, :] = acc[0:2]
        before = before + jnp.where(p < mine, got, 0.0)
        acc = acc + got
    number = jnp.where(mine < FAR // 2, acc[2:3], acc[3:4])
    closing = acc[0:2] / jnp.maximum(number, 1.0)
    for p in range(FAR):
        out[p, 2:4, :] = closing
    counts_out[0:2, :] = before[2:4]


def start_kernel(far, arrived, counts, out_far, closing, out, buf, sems):
    for p in range(FAR):
        buf[2 * p : 2 * p + 2, :] = far[p, 0:2, :]
        closing[2 * p : 2 * p + 2, :] = far[p, 2:4, :]
    buf[128:130, :] = counts[0:2, :]
    buf[130:136, :] = jnp.zeros((6, LANES), F32)
    acc = buf[...]
    copies = []
    for k in range(SIB):
        i = 2 * (k % 4) + k // 4
        out[i] = acc
        copies.append(pltpu.make_async_copy(out.at[i], out_far.at[i], sems.at[i]))
        copies[-1].start()
        acc = acc + arrived[i]
    for copy in copies:
        copy.wait()


def both(slot, j):
    return jnp.concatenate([slot[2 * j : 2 * j + 1, :], slot[2 * j + 1 : 2 * j + 2, :]], axis=1)


def own_kernel(split, slot, cols, out, local):
    local[...] = split[0:LHS, :] + split[LHS : 2 * LHS, :]
    label = lax.broadcasted_iota(jnp.int32, (T, T), 0)
    order = label <= lax.broadcasted_iota(jnp.int32, (T, T), 1)
    for j in range(NT):
        row = jnp.broadcast_to(both(slot, j), (T, T))
        own = None
        for k in range(j + 1):
            at = slice(k * T, (k + 1) * T)
            keys = cols[at, :]
            mask = jnp.concatenate([keys, keys], axis=1) == row
            if k == j:
                mask = jnp.logical_and(mask, order)
            part = dot(local[:, at], hot(mask))
            own = part if own is None else own + part
        at = slice(j * T, (j + 1) * T)
        out[0:64, at] = own[0:64] + own[64:128]
        out[64:72, at] = own[128:136]


def running_kernel(start, own, slot, closed, mean, count_far, closing_far, left, held_mean, count, closing, sems):
    for c in range(2):
        for h in range(2):
            closing[:, c * T + h * LANES : c * T + (h + 1) * LANES] = closed[c, h * 64 : (h + 1) * 64, :]
    copies = [pltpu.make_async_copy(closing, closing_far, sems.at[NT])]
    copies[0].start()
    sub = lax.broadcasted_iota(jnp.int32, (16, LANES), 0)
    for j in range(NT):
        for h in range(2):
            a, b, _ = pieces(start[j, h * 64 : (h + 1) * 64, :])
            n = pieces(start[j, 128 + h : 129 + h, :])
            n = [jnp.broadcast_to(v.astype(F32), (16, LANES)) for v in n]
            n = jnp.where(sub == 0, n[0], jnp.where(sub == 1, n[1], jnp.where(sub == 2, n[2], 0.0)))
            top = (j // NH) * LHS
            at = (j % NH) * T + h * LANES
            left[top : top + LHS, at : at + LANES] = jnp.concatenate([a, b, n.astype(BF16)], axis=0)
    label = lax.broadcasted_iota(jnp.int32, (T, T), 0)
    for j in range(NT):
        row = both(slot, j)
        high = jnp.broadcast_to(row, (LHS, T)) >= HALF
        low = jnp.bitwise_and(jnp.broadcast_to(row, (T, T)), HALF - 1)
        res = None
        for k in range(NH):
            part = dot(left[:, k * T : (k + 1) * T], hot(label + k * T == low))
            res = part if res is None else res + part
        res = jnp.where(high, res[LHS : 2 * LHS], res[0:LHS])
        at = slice(j * T, (j + 1) * T)
        total = res[0:64] + res[64:128] + own[0:64, at]
        tally = (res[128:129] + res[129:130]) + res[130:131] + own[64:65, at]
        held_mean[:, at] = total / tally
        copies.append(pltpu.make_async_copy(held_mean.at[:, at], mean.at[:, at], sems.at[j]))
        copies[-1].start()
        whole = tally.astype(jnp.int32)
        count[2 * j : 2 * j + 1, :] = whole[:, :LANES]
        count[2 * j + 1 : 2 * j + 2, :] = whole[:, LANES:]
    copies.append(pltpu.make_async_copy(count, count_far, sems.at[NT + 1]))
    copies[-1].start()
    for copy in copies:
        copy.wait()


def shape(*dims, dtype=F32):
    return jax.ShapeDtypeStruct(dims, dtype)


def near(*dims, dtype=F32):
    return pltpu.VMEM(dims, dtype)


def outward(*dims):
    return pltpu.HBM(dims, F32)


def outer(x):
    return pltpu.with_memory_space_constraint(x, pltpu.HBM)


def held(x):
    return pltpu.with_memory_space_constraint(x, pltpu.VMEM)


def sums_call(vt, gid, table):
    outside = pl.BlockSpec(memory_space=pl.ANY)
    return pl.pallas_call(
        sums_kernel,
        in_specs=[outside] * 3,
        out_shape=(
            near(SIB, MSG, LANES),
            near(16, LANES, dtype=jnp.int32),
            near(2 * LHS, R, dtype=BF16),
            near(R, LANES, dtype=jnp.int32),
        ),
        scratch_shapes=[
            pltpu.VMEM((M, R), F32),
            pltpu.VMEM((16, LANES), jnp.int32),
            pltpu.VMEM((16, LANES), jnp.int32),
            pltpu.SemaphoreType.DMA((7,)),
        ],
        compiler_params=ROOM,
        name="local_sums",
    )(outer(vt), outer(gid), outer(table))


def own_call(split, slot, cols):
    return pl.pallas_call(
        own_kernel,
        out_shape=near(72, R),
        scratch_shapes=[pltpu.VMEM((LHS, R), BF16)],
        compiler_params=ROOM,
        cost_estimate=pl.CostEstimate(flops=2 * 144 * R * R // 2, bytes_accessed=1 << 20, transcendentals=0),
        name="own_rows",
    )(held(split), held(slot), held(cols))


def running_call(start, own, slot, closed):
    return pl.pallas_call(
        running_kernel,
        out_shape=(shape(M, R), shape(16, LANES, dtype=jnp.int32), shape(M, 512)),
        out_specs=(pl.BlockSpec(memory_space=pl.ANY),) * 3,
        scratch_shapes=[
            pltpu.VMEM((2 * LHS, HALF), BF16),
            pltpu.VMEM((M, R), F32),
            pltpu.VMEM((16, LANES), jnp.int32),
            pltpu.VMEM((M, 2 * T), F32),
            pltpu.SemaphoreType.DMA((NT + 2,)),
        ],
        compiler_params=ROOM,
        name="running_means",
    )(start, held(own), held(slot), closed)


def local(values, group_ids, slot_of):
    vt = values.T
    gid = group_ids.reshape(16, LANES)
    table = slot_of.reshape(16, LANES)
    sums, slot, split, cols = sums_call(vt, gid, table)
    siblings = ("x", "c")
    arrived = held(lax.all_to_all(sums, siblings, 0, 0, tiled=True))
    far = ("y", "z")
    pieces_out = pl.pallas_call(
        slice_kernel,
        out_shape=near(FAR, 4, LANES),
        scratch_shapes=[pltpu.VMEM((MSG, LANES), F32)],
        compiler_params=ROOM,
        name="slice_sums",
    )(arrived)
    met = held(lax.all_to_all(pieces_out, far, 0, 0, tiled=True))
    scanned, counts = pl.pallas_call(
        scan_kernel,
        out_shape=(near(FAR, 4, LANES), near(8, LANES)),
        compiler_params=ROOM,
        name="scan",
    )(met)
    back = held(lax.all_to_all(scanned, far, 0, 0, tiled=True))
    starts, closing_half = pl.pallas_call(
        start_kernel,
        out_shape=(outward(SIB, MSG, LANES), near(LANES, LANES)),
        out_specs=(pl.BlockSpec(memory_space=pl.ANY), pl.BlockSpec(memory_space=pltpu.VMEM)),
        scratch_shapes=[
            pltpu.VMEM((SIB, MSG, LANES), F32),
            pltpu.VMEM((MSG, LANES), F32),
            pltpu.SemaphoreType.DMA((SIB,)),
        ],
        compiler_params=ROOM,
        name="starts",
    )(back, arrived, counts)
    closed = held(lax.all_gather(closing_half, "c"))
    own = own_call(split, slot, cols)
    start = held(lax.all_to_all(starts, siblings, 0, 0, tiled=True))
    mean, count, closing = running_call(start, own, slot, closed)
    return mean.T, count.reshape(R), closing.T


def solution(mesh):
    split = Mesh(mesh.devices.reshape(8, 8, 2, 4), ROWS_ALL)
    in_specs = (P(ROWS_ALL, None), P(ROWS_ALL), P())
    out_specs = (P(ROWS_ALL, None), P(ROWS_ALL), P("x", None))
    return jax.shard_map(local, mesh=split, in_specs=in_specs, out_specs=out_specs, check_vma=False)
```

```python
import jax
import jax.numpy as jnp
from jax import lax
from jax.experimental import pallas as pl
from jax.experimental.pallas import tpu as pltpu
from jax.sharding import Mesh
from jax.sharding import PartitionSpec as P

ROWS_ALL = ("y", "z", "c", "x")
F32 = jnp.float32
BF16 = jnp.bfloat16
M = 64
R = 2048
S = 2048
LANES = 128
T = 256
NT = S // T
NH = NT // 2
WAYS = 4
PART = S // WAYS
NW = NT // WAYS
SIB = 8
FAR = 64
MSG = 136
LHS = 144
HALF = 1024


ROOM = pltpu.CompilerParams(vmem_limit_bytes=16 << 20)


def pieces(v):
    a = v.astype(BF16)
    rest = v - a.astype(F32)
    b = rest.astype(BF16)
    c = (rest - b.astype(F32)).astype(BF16)
    return a, b, c


def lookup(table, idx):
    low = jnp.bitwise_and(idx, LANES - 1)
    high = jnp.right_shift(idx, 7)
    out = jnp.zeros_like(idx)
    for k in range(S // LANES):
        row = jnp.broadcast_to(table[k : k + 1, :], idx.shape)
        out = jnp.where(high == k, jnp.take_along_axis(row, low, axis=1), out)
    return out


def columns(slot):
    flipped = jnp.concatenate([slot] * 8, axis=0).T
    return [jnp.broadcast_to(flipped[:, i : i + 1], (LANES, LANES)) for i in range(R // LANES)]


def dot(a, b):
    return lax.dot_general(a, b, (((1,), (0,)), ((), ())), preferred_element_type=F32)


def owner(block):
    return 4 * (block % 2) + block // 2


def hot(mask):
    return jnp.where(mask, 1.0, 0.0).astype(BF16)


def sums_kernel(vt_far, gid_far, table_far, out, slot_out, split, cols, vt, gid, table, sems):
    values_in = [
        pltpu.make_async_copy(vt_far.at[16 * g : 16 * g + 16], vt.at[16 * g : 16 * g + 16], sems.at[3 + g]) for g in range(4)
    ]
    keys_in = pltpu.make_async_copy(gid_far, gid, sems.at[1])
    table_in = pltpu.make_async_copy(table_far, table, sems.at[2])
    keys_in.start()
    table_in.start()
    for copy in values_in:
        copy.start()
    keys_in.wait()
    table_in.wait()
    slot = lookup(table[...], gid[...])
    slot_out[...] = slot
    sub = lax.broadcasted_iota(jnp.int32, (16, LANES), 0)
    ones = jnp.where(sub == 0, 1.0, 0.0).astype(BF16)
    spans = [slice(i * LANES, (i + 1) * LANES) for i in range(R // LANES)]
    high = jnp.where(slot >= HALF, 1.0, 0.0)
    highs = [jnp.broadcast_to(high[i : i + 1, :], (16, LANES)) for i in range(R // LANES)]
    picks = [((1.0 - h).astype(BF16), h.astype(BF16)) for h in highs]

    def place(rows, at, value, pick):
        split[rows : rows + 16, at] = value * pick[0]
        split[LHS + rows : LHS + rows + 16, at] = value * pick[1]

    for at, pick in zip(spans, picks):
        place(128, at, ones, pick)
    for g in range(4):
        values_in[g].wait()
        for at, pick in zip(spans, picks):
            a, b, _ = pieces(vt[16 * g : 16 * g + 16, at])
            place(16 * g, at, a, pick)
            place(64 + 16 * g, at, b, pick)
    for i, block in enumerate(columns(slot)):
        cols[i * LANES : (i + 1) * LANES, :] = block
    lane = lax.broadcasted_iota(jnp.int32, (T, T), 1)
    first = lax.broadcasted_iota(jnp.int32, (8, LANES), 0) == 0
    for j in range(NH):
        res = None
        for k in range(NT):
            at = slice(k * T, (k + 1) * T)
            keys = jnp.bitwise_and(cols[at, :], HALF - 1)
            keys = jnp.concatenate([keys, keys], axis=1)
            part = dot(split[:, at], hot(keys == lane + j * T))
            res = part if res is None else res + part
        for h in range(2):
            of = res[h * LHS : (h + 1) * LHS]
            total = of[0:64] + of[64:128]
            to = owner(h * NH + j)
            out[to, 0:64, :] = total[:, :LANES]
            out[to, 64:128, :] = total[:, LANES:]
            number = jnp.broadcast_to(of[128:129], (8, T))
            out[to, 128:136, :] = jnp.where(first, number[:, :LANES], number[:, LANES:])


def slice_kernel(arrived, out, buf):
    total = arrived[0]
    for i in range(1, SIB):
        total = total + arrived[i]
    buf[...] = total
    counts = buf[128:130, :]
    for p in range(FAR):
        out[p, 0:2, :] = buf[2 * p : 2 * p + 2, :]
        out[p, 2:4, :] = counts


def scan_kernel(arrived, out, counts_out):
    mine = lax.axis_index("y") * 8 + lax.axis_index("z")
    acc = jnp.zeros((4, LANES), F32)
    before = jnp.zeros((4, LANES), F32)
    for p in range(FAR):
        got = arrived[p]
        out[p, 0:2, :] = acc[0:2]
        before = before + jnp.where(p < mine, got, 0.0)
        acc = acc + got
    number = jnp.where(mine < FAR // 2, acc[2:3], acc[3:4])
    closing = acc[0:2] / jnp.maximum(number, 1.0)
    for p in range(FAR):
        out[p, 2:4, :] = closing
    counts_out[0:2, :] = before[2:4]


def start_kernel(far, arrived, counts, out_far, closing, out, buf, sems):
    for p in range(FAR):
        buf[2 * p : 2 * p + 2, :] = far[p, 0:2, :]
        closing[2 * p : 2 * p + 2, :] = far[p, 2:4, :]
    buf[128:130, :] = counts[0:2, :]
    buf[130:136, :] = jnp.zeros((6, LANES), F32)
    acc = buf[...]
    copies = []
    for k in range(SIB):
        out[k] = acc
        copies.append(pltpu.make_async_copy(out.at[k], out_far.at[k], sems.at[k]))
        copies[-1].start()
        acc = acc + arrived[k]
    for copy in copies:
        copy.wait()


def both(slot, j):
    return jnp.concatenate([slot[2 * j : 2 * j + 1, :], slot[2 * j + 1 : 2 * j + 2, :]], axis=1)


def own_kernel(split, slot, cols, out, local):
    local[...] = split[0:LHS, :] + split[LHS : 2 * LHS, :]
    label = lax.broadcasted_iota(jnp.int32, (T, T), 0)
    order = label <= lax.broadcasted_iota(jnp.int32, (T, T), 1)
    for j in range(NT):
        row = jnp.broadcast_to(both(slot, j), (T, T))
        own = None
        for k in range(j + 1):
            at = slice(k * T, (k + 1) * T)
            keys = cols[at, :]
            mask = jnp.concatenate([keys, keys], axis=1) == row
            if k == j:
                mask = jnp.logical_and(mask, order)
            part = dot(local[:, at], hot(mask))
            own = part if own is None else own + part
        at = slice(j * T, (j + 1) * T)
        out[0:64, at] = own[0:64] + own[64:128]
        out[64:72, at] = own[128:136]


def running_kernel(start, own, slot, closed, mean, count_far, closing_far, left, held_mean, count, closing, sems):
    for c in range(2):
        for h in range(2):
            closing[:, c * T + h * LANES : c * T + (h + 1) * LANES] = closed[c, h * 64 : (h + 1) * 64, :]
    copies = [pltpu.make_async_copy(closing, closing_far, sems.at[NT])]
    copies[0].start()
    sub = lax.broadcasted_iota(jnp.int32, (16, LANES), 0)
    for j in range(NT):
        for h in range(2):
            a, b, _ = pieces(start[owner(j), h * 64 : (h + 1) * 64, :])
            n = pieces(start[owner(j), 128 + h : 129 + h, :])
            n = [jnp.broadcast_to(v.astype(F32), (16, LANES)) for v in n]
            n = jnp.where(sub == 0, n[0], jnp.where(sub == 1, n[1], jnp.where(sub == 2, n[2], 0.0)))
            top = (j // NW) * LHS
            at = (j % NW) * T + h * LANES
            left[top : top + LHS, at : at + LANES] = jnp.concatenate([a, b, n.astype(BF16)], axis=0)
    label = lax.broadcasted_iota(jnp.int32, (T, T), 0)
    for j in range(NT):
        row = both(slot, j)
        high = jnp.broadcast_to(jnp.right_shift(row, 9), (LHS, T))
        low = jnp.bitwise_and(jnp.broadcast_to(row, (T, T)), PART - 1)
        res = None
        for k in range(NW):
            part = dot(left[:, k * T : (k + 1) * T], hot(label + k * T == low))
            res = part if res is None else res + part
        found = res[0:LHS]
        for w in range(1, WAYS):
            found = jnp.where(high == w, res[w * LHS : (w + 1) * LHS], found)
        res = found
        at = slice(j * T, (j + 1) * T)
        total = res[0:64] + res[64:128] + own[0:64, at]
        tally = (res[128:129] + res[129:130]) + res[130:131] + own[64:65, at]
        held_mean[:, at] = total / tally
        copies.append(pltpu.make_async_copy(held_mean.at[:, at], mean.at[:, at], sems.at[j]))
        copies[-1].start()
        whole = tally.astype(jnp.int32)
        count[2 * j : 2 * j + 1, :] = whole[:, :LANES]
        count[2 * j + 1 : 2 * j + 2, :] = whole[:, LANES:]
    copies.append(pltpu.make_async_copy(count, count_far, sems.at[NT + 1]))
    copies[-1].start()
    for copy in copies:
        copy.wait()


def shape(*dims, dtype=F32):
    return jax.ShapeDtypeStruct(dims, dtype)


def near(*dims, dtype=F32):
    return pltpu.VMEM(dims, dtype)


def outward(*dims):
    return pltpu.HBM(dims, F32)


def outer(x):
    return pltpu.with_memory_space_constraint(x, pltpu.HBM)


def held(x):
    return pltpu.with_memory_space_constraint(x, pltpu.VMEM)


def sums_call(vt, gid, table):
    outside = pl.BlockSpec(memory_space=pl.ANY)
    return pl.pallas_call(
        sums_kernel,
        in_specs=[outside] * 3,
        out_shape=(
            near(SIB, MSG, LANES),
            near(16, LANES, dtype=jnp.int32),
            near(2 * LHS, R, dtype=BF16),
            near(R, LANES, dtype=jnp.int32),
        ),
        scratch_shapes=[
            pltpu.VMEM((M, R), F32),
            pltpu.VMEM((16, LANES), jnp.int32),
            pltpu.VMEM((16, LANES), jnp.int32),
            pltpu.SemaphoreType.DMA((7,)),
        ],
        compiler_params=ROOM,
        name="local_sums",
    )(outer(vt), outer(gid), outer(table))


def own_call(split, slot, cols):
    return pl.pallas_call(
        own_kernel,
        out_shape=near(72, R),
        scratch_shapes=[pltpu.VMEM((LHS, R), BF16)],
        compiler_params=ROOM,
        cost_estimate=pl.CostEstimate(flops=2 * 144 * R * R // 2, bytes_accessed=1 << 20, transcendentals=0),
        name="own_rows",
    )(held(split), held(slot), held(cols))


def running_call(start, own, slot, closed):
    return pl.pallas_call(
        running_kernel,
        out_shape=(shape(M, R), shape(16, LANES, dtype=jnp.int32), shape(M, 512)),
        out_specs=(pl.BlockSpec(memory_space=pl.ANY),) * 3,
        scratch_shapes=[
            pltpu.VMEM((WAYS * LHS, PART), BF16),
            pltpu.VMEM((M, R), F32),
            pltpu.VMEM((16, LANES), jnp.int32),
            pltpu.VMEM((M, 2 * T), F32),
            pltpu.SemaphoreType.DMA((NT + 2,)),
        ],
        compiler_params=ROOM,
        name="running_means",
    )(start, held(own), held(slot), closed)


def local(values, group_ids, slot_of):
    vt = values.T
    gid = group_ids.reshape(16, LANES)
    table = slot_of.reshape(16, LANES)
    sums, slot, split, cols = sums_call(vt, gid, table)
    siblings = ("c", "x")
    arrived = held(lax.all_to_all(sums, siblings, 0, 0, tiled=True))
    far = ("y", "z")
    pieces_out = pl.pallas_call(
        slice_kernel,
        out_shape=near(FAR, 4, LANES),
        scratch_shapes=[pltpu.VMEM((MSG, LANES), F32)],
        compiler_params=ROOM,
        name="slice_sums",
    )(arrived)
    met = held(lax.all_to_all(pieces_out, far, 0, 0, tiled=True))
    scanned, counts = pl.pallas_call(
        scan_kernel,
        out_shape=(near(FAR, 4, LANES), near(8, LANES)),
        compiler_params=ROOM,
        name="scan",
    )(met)
    back = held(lax.all_to_all(scanned, far, 0, 0, tiled=True))
    starts, closing_half = pl.pallas_call(
        start_kernel,
        out_shape=(outward(SIB, MSG, LANES), near(LANES, LANES)),
        out_specs=(pl.BlockSpec(memory_space=pl.ANY), pl.BlockSpec(memory_space=pltpu.VMEM)),
        scratch_shapes=[
            pltpu.VMEM((SIB, MSG, LANES), F32),
            pltpu.VMEM((MSG, LANES), F32),
            pltpu.SemaphoreType.DMA((SIB,)),
        ],
        compiler_params=ROOM,
        name="starts",
    )(back, arrived, counts)
    closed = held(lax.all_gather(closing_half, "c"))
    own = own_call(split, slot, cols)
    start = held(lax.all_to_all(starts, siblings, 0, 0, tiled=True))
    mean, count, closing = running_call(start, own, slot, closed)
    return mean.T, count.reshape(R), closing.T


def solution(mesh):
    split = Mesh(mesh.devices.reshape(8, 8, 2, 4), ROWS_ALL)
    in_specs = (P(ROWS_ALL, None), P(ROWS_ALL), P())
    out_specs = (P(ROWS_ALL, None), P(ROWS_ALL), P("x", None))
    return jax.shard_map(local, mesh=split, in_specs=in_specs, out_specs=out_specs, check_vma=False)
```

```python
import jax
import jax.numpy as jnp
from jax import lax
from jax.experimental import pallas as pl
from jax.experimental.pallas import tpu as pltpu
from jax.sharding import Mesh
from jax.sharding import PartitionSpec as P

ROWS_ALL = ("y", "z", "c", "x")
F32 = jnp.float32
BF16 = jnp.bfloat16
M = 64
R = 2048
S = 2048
LANES = 128
T = 256
NT = S // T
NH = NT // 2
WAYS = 4
PART = S // WAYS
NW = NT // WAYS
SIB = 8
FAR = 64
MSG = 136
LHS = 144
HALF = 1024


ROOM = pltpu.CompilerParams(vmem_limit_bytes=16 << 20)


def pieces(v):
    a = v.astype(BF16)
    rest = v - a.astype(F32)
    b = rest.astype(BF16)
    c = (rest - b.astype(F32)).astype(BF16)
    return a, b, c


def lookup(table, idx):
    low = jnp.bitwise_and(idx, LANES - 1)
    high = jnp.right_shift(idx, 7)
    out = jnp.zeros_like(idx)
    for k in range(S // LANES):
        row = jnp.broadcast_to(table[k : k + 1, :], idx.shape)
        out = jnp.where(high == k, jnp.take_along_axis(row, low, axis=1), out)
    return out


def columns(slot):
    flipped = jnp.concatenate([slot] * 8, axis=0).T
    return [jnp.broadcast_to(flipped[:, i : i + 1], (LANES, LANES)) for i in range(R // LANES)]


def dot(a, b):
    return lax.dot_general(a, b, (((1,), (0,)), ((), ())), preferred_element_type=F32)


def owner(block):
    return 4 * (block % 2) + block // 2


def hot(mask):
    return jnp.where(mask, 1.0, 0.0).astype(BF16)


def sums_kernel(vt_far, gid_far, table_far, out, slot_out, split, cols, vt, gid, table, sems):
    values_in = [
        pltpu.make_async_copy(vt_far.at[16 * g : 16 * g + 16], vt.at[16 * g : 16 * g + 16], sems.at[3 + g]) for g in range(4)
    ]
    keys_in = pltpu.make_async_copy(gid_far, gid, sems.at[1])
    table_in = pltpu.make_async_copy(table_far, table, sems.at[2])
    keys_in.start()
    table_in.start()
    for copy in values_in:
        copy.start()
    keys_in.wait()
    table_in.wait()
    slot = lookup(table[...], gid[...])
    slot_out[...] = slot
    sub = lax.broadcasted_iota(jnp.int32, (16, LANES), 0)
    ones = jnp.where(sub == 0, 1.0, 0.0).astype(BF16)
    spans = [slice(i * LANES, (i + 1) * LANES) for i in range(R // LANES)]
    high = jnp.where(slot >= HALF, 1.0, 0.0)
    highs = [jnp.broadcast_to(high[i : i + 1, :], (16, LANES)) for i in range(R // LANES)]
    picks = [((1.0 - h).astype(BF16), h.astype(BF16)) for h in highs]

    def place(rows, at, value, pick):
        split[rows : rows + 16, at] = value * pick[0]
        split[LHS + rows : LHS + rows + 16, at] = value * pick[1]

    for at, pick in zip(spans, picks):
        place(128, at, ones, pick)
    for g in range(4):
        values_in[g].wait()
        for at, pick in zip(spans, picks):
            a, b, _ = pieces(vt[16 * g : 16 * g + 16, at])
            place(16 * g, at, a, pick)
            place(64 + 16 * g, at, b, pick)
    for i, block in enumerate(columns(slot)):
        cols[i * LANES : (i + 1) * LANES, :] = block
    lane = lax.broadcasted_iota(jnp.int32, (T, T), 1)
    first = lax.broadcasted_iota(jnp.int32, (8, LANES), 0) == 0
    for j in range(NH):
        res = None
        for k in range(NT):
            at = slice(k * T, (k + 1) * T)
            keys = jnp.bitwise_and(cols[at, :], HALF - 1)
            keys = jnp.concatenate([keys, keys], axis=1)
            part = dot(split[:, at], hot(keys == lane + j * T))
            res = part if res is None else res + part
        for h in range(2):
            of = res[h * LHS : (h + 1) * LHS]
            total = of[0:64] + of[64:128]
            to = owner(h * NH + j)
            out[to, 0:64, :] = total[:, :LANES]
            out[to, 64:128, :] = total[:, LANES:]
            number = jnp.broadcast_to(of[128:129], (8, T))
            out[to, 128:136, :] = jnp.where(first, number[:, :LANES], number[:, LANES:])


def slice_kernel(arrived, out, buf):
    total = arrived[0]
    for i in range(1, SIB):
        total = total + arrived[i]
    buf[...] = total
    counts = buf[128:130, :]
    for p in range(FAR):
        out[p, 0:2, :] = buf[2 * p : 2 * p + 2, :]
        out[p, 2:4, :] = counts


def scan_kernel(arrived, out, counts_out):
    y = lax.axis_index("y")
    z = lax.axis_index("z")
    mine = y * 8 + z
    acc = jnp.zeros((4, LANES), F32)
    before = jnp.zeros((4, LANES), F32)
    for r in range(FAR):
        p = 8 * (r % 8) + r // 8
        got = arrived[p]
        out[p, 0:2, :] = acc[0:2]
        before = before + jnp.where(r < mine, got, 0.0)
        acc = acc + got
    number = jnp.where(z < 4, acc[2:3], acc[3:4])
    closing = acc[0:2] / jnp.maximum(number, 1.0)
    for p in range(FAR):
        out[p, 2:4, :] = closing
    counts_out[0:2, :] = before[2:4]


def start_kernel(far, arrived, counts, out_far, closing, out, buf, sems):
    for p in range(FAR):
        buf[2 * p : 2 * p + 2, :] = far[p, 0:2, :]
        closing[2 * p : 2 * p + 2, :] = far[p, 2:4, :]
    buf[128:130, :] = counts[0:2, :]
    buf[130:136, :] = jnp.zeros((6, LANES), F32)
    acc = buf[...]
    copies = []
    for k in range(SIB):
        out[k] = acc
        copies.append(pltpu.make_async_copy(out.at[k], out_far.at[k], sems.at[k]))
        copies[-1].start()
        acc = acc + arrived[k]
    for copy in copies:
        copy.wait()


def both(slot, j):
    return jnp.concatenate([slot[2 * j : 2 * j + 1, :], slot[2 * j + 1 : 2 * j + 2, :]], axis=1)


def own_kernel(split, slot, cols, out, local):
    local[...] = split[0:LHS, :] + split[LHS : 2 * LHS, :]
    label = lax.broadcasted_iota(jnp.int32, (T, T), 0)
    order = label <= lax.broadcasted_iota(jnp.int32, (T, T), 1)
    for j in range(NT):
        row = jnp.broadcast_to(both(slot, j), (T, T))
        own = None
        for k in range(j + 1):
            at = slice(k * T, (k + 1) * T)
            keys = cols[at, :]
            mask = jnp.concatenate([keys, keys], axis=1) == row
            if k == j:
                mask = jnp.logical_and(mask, order)
            part = dot(local[:, at], hot(mask))
            own = part if own is None else own + part
        at = slice(j * T, (j + 1) * T)
        out[0:64, at] = own[0:64] + own[64:128]
        out[64:72, at] = own[128:136]


def running_kernel(start, own, slot, closed, mean, count_far, closing_far, left, held_mean, count, closing, sems):
    for c in range(2):
        for h in range(2):
            closing[:, c * T + h * LANES : c * T + (h + 1) * LANES] = closed[c, h * 64 : (h + 1) * 64, :]
    copies = [pltpu.make_async_copy(closing, closing_far, sems.at[NT])]
    copies[0].start()
    sub = lax.broadcasted_iota(jnp.int32, (16, LANES), 0)
    for j in range(NT):
        for h in range(2):
            a, b, _ = pieces(start[owner(j), h * 64 : (h + 1) * 64, :])
            n = pieces(start[owner(j), 128 + h : 129 + h, :])
            n = [jnp.broadcast_to(v.astype(F32), (16, LANES)) for v in n]
            n = jnp.where(sub == 0, n[0], jnp.where(sub == 1, n[1], jnp.where(sub == 2, n[2], 0.0)))
            top = (j // NW) * LHS
            at = (j % NW) * T + h * LANES
            left[top : top + LHS, at : at + LANES] = jnp.concatenate([a, b, n.astype(BF16)], axis=0)
    label = lax.broadcasted_iota(jnp.int32, (T, T), 0)
    for j in range(NT):
        row = both(slot, j)
        high = jnp.broadcast_to(jnp.right_shift(row, 9), (LHS, T))
        low = jnp.bitwise_and(jnp.broadcast_to(row, (T, T)), PART - 1)
        res = None
        for k in range(NW):
            part = dot(left[:, k * T : (k + 1) * T], hot(label + k * T == low))
            res = part if res is None else res + part
        found = res[0:LHS]
        for w in range(1, WAYS):
            found = jnp.where(high == w, res[w * LHS : (w + 1) * LHS], found)
        res = found
        at = slice(j * T, (j + 1) * T)
        total = res[0:64] + res[64:128] + own[0:64, at]
        tally = (res[128:129] + res[129:130]) + res[130:131] + own[64:65, at]
        held_mean[:, at] = total / tally
        copies.append(pltpu.make_async_copy(held_mean.at[:, at], mean.at[:, at], sems.at[j]))
        copies[-1].start()
        whole = tally.astype(jnp.int32)
        count[2 * j : 2 * j + 1, :] = whole[:, :LANES]
        count[2 * j + 1 : 2 * j + 2, :] = whole[:, LANES:]
    copies.append(pltpu.make_async_copy(count, count_far, sems.at[NT + 1]))
    copies[-1].start()
    for copy in copies:
        copy.wait()


def shape(*dims, dtype=F32):
    return jax.ShapeDtypeStruct(dims, dtype)


def near(*dims, dtype=F32):
    return pltpu.VMEM(dims, dtype)


def outward(*dims):
    return pltpu.HBM(dims, F32)


def outer(x):
    return pltpu.with_memory_space_constraint(x, pltpu.HBM)


def held(x):
    return pltpu.with_memory_space_constraint(x, pltpu.VMEM)


def sums_call(vt, gid, table):
    outside = pl.BlockSpec(memory_space=pl.ANY)
    return pl.pallas_call(
        sums_kernel,
        in_specs=[outside] * 3,
        out_shape=(
            near(SIB, MSG, LANES),
            near(16, LANES, dtype=jnp.int32),
            near(2 * LHS, R, dtype=BF16),
            near(R, LANES, dtype=jnp.int32),
        ),
        scratch_shapes=[
            pltpu.VMEM((M, R), F32),
            pltpu.VMEM((16, LANES), jnp.int32),
            pltpu.VMEM((16, LANES), jnp.int32),
            pltpu.SemaphoreType.DMA((7,)),
        ],
        compiler_params=ROOM,
        name="local_sums",
    )(outer(vt), outer(gid), outer(table))


def own_call(split, slot, cols):
    return pl.pallas_call(
        own_kernel,
        out_shape=near(72, R),
        scratch_shapes=[pltpu.VMEM((LHS, R), BF16)],
        compiler_params=ROOM,
        cost_estimate=pl.CostEstimate(flops=2 * 144 * R * R // 2, bytes_accessed=1 << 20, transcendentals=0),
        name="own_rows",
    )(held(split), held(slot), held(cols))


def running_call(start, own, slot, closed):
    return pl.pallas_call(
        running_kernel,
        out_shape=(shape(M, R), shape(16, LANES, dtype=jnp.int32), shape(M, 512)),
        out_specs=(pl.BlockSpec(memory_space=pl.ANY),) * 3,
        scratch_shapes=[
            pltpu.VMEM((WAYS * LHS, PART), BF16),
            pltpu.VMEM((M, R), F32),
            pltpu.VMEM((16, LANES), jnp.int32),
            pltpu.VMEM((M, 2 * T), F32),
            pltpu.SemaphoreType.DMA((NT + 2,)),
        ],
        compiler_params=ROOM,
        name="running_means",
    )(start, held(own), held(slot), closed)


def local(values, group_ids, slot_of):
    vt = values.T
    gid = group_ids.reshape(16, LANES)
    table = slot_of.reshape(16, LANES)
    sums, slot, split, cols = sums_call(vt, gid, table)
    siblings = ("c", "x")
    arrived = held(lax.all_to_all(sums, siblings, 0, 0, tiled=True))
    far = ("z", "y")
    pieces_out = pl.pallas_call(
        slice_kernel,
        out_shape=near(FAR, 4, LANES),
        scratch_shapes=[pltpu.VMEM((MSG, LANES), F32)],
        compiler_params=ROOM,
        name="slice_sums",
    )(arrived)
    met = held(lax.all_to_all(pieces_out, far, 0, 0, tiled=True))
    scanned, counts = pl.pallas_call(
        scan_kernel,
        out_shape=(near(FAR, 4, LANES), near(8, LANES)),
        compiler_params=ROOM,
        name="scan",
    )(met)
    back = held(lax.all_to_all(scanned, far, 0, 0, tiled=True))
    starts, closing_half = pl.pallas_call(
        start_kernel,
        out_shape=(outward(SIB, MSG, LANES), near(LANES, LANES)),
        out_specs=(pl.BlockSpec(memory_space=pl.ANY), pl.BlockSpec(memory_space=pltpu.VMEM)),
        scratch_shapes=[
            pltpu.VMEM((SIB, MSG, LANES), F32),
            pltpu.VMEM((MSG, LANES), F32),
            pltpu.SemaphoreType.DMA((SIB,)),
        ],
        compiler_params=ROOM,
        name="starts",
    )(back, arrived, counts)
    closed = held(lax.all_gather(closing_half, "c"))
    own = own_call(split, slot, cols)
    start = held(lax.all_to_all(starts, siblings, 0, 0, tiled=True))
    mean, count, closing = running_call(start, own, slot, closed)
    return mean.T, count.reshape(R), closing.T


def solution(mesh):
    split = Mesh(mesh.devices.reshape(8, 8, 2, 4), ROWS_ALL)
    in_specs = (P(ROWS_ALL, None), P(ROWS_ALL), P())
    out_specs = (P(ROWS_ALL, None), P(ROWS_ALL), P("x", None))
    return jax.shard_map(local, mesh=split, in_specs=in_specs, out_specs=out_specs, check_vma=False)
```

```python
import jax
import jax.numpy as jnp
from jax import lax
from jax.experimental import pallas as pl
from jax.experimental.pallas import tpu as pltpu
from jax.sharding import Mesh
from jax.sharding import PartitionSpec as P

ROWS_ALL = ("y", "z", "c", "x")
F32 = jnp.float32
BF16 = jnp.bfloat16
M = 64
R = 2048
S = 2048
LANES = 128
T = 256
NT = S // T
NH = NT // 2
WAYS = 4
PART = S // WAYS
NW = NT // WAYS
SIB = 8
RING = 8
MSG = 136
LHS = 144
HALF = 1024


ROOM = pltpu.CompilerParams(vmem_limit_bytes=16 << 20)


def pieces(v):
    a = v.astype(BF16)
    rest = v - a.astype(F32)
    b = rest.astype(BF16)
    c = (rest - b.astype(F32)).astype(BF16)
    return a, b, c


def lookup(table, idx):
    low = jnp.bitwise_and(idx, LANES - 1)
    high = jnp.right_shift(idx, 7)
    out = jnp.zeros_like(idx)
    for k in range(S // LANES):
        row = jnp.broadcast_to(table[k : k + 1, :], idx.shape)
        out = jnp.where(high == k, jnp.take_along_axis(row, low, axis=1), out)
    return out


def columns(slot):
    flipped = jnp.concatenate([slot] * 8, axis=0).T
    return [jnp.broadcast_to(flipped[:, i : i + 1], (LANES, LANES)) for i in range(R // LANES)]


def dot(a, b):
    return lax.dot_general(a, b, (((1,), (0,)), ((), ())), preferred_element_type=F32)


def owner(block):
    return 4 * (block % 2) + block // 2


def hot(mask):
    return jnp.where(mask, 1.0, 0.0).astype(BF16)


def sums_kernel(vt_far, gid_far, table_far, out, slot_out, split, cols, vt, gid, table, sems):
    values_in = [
        pltpu.make_async_copy(vt_far.at[16 * g : 16 * g + 16], vt.at[16 * g : 16 * g + 16], sems.at[3 + g]) for g in range(4)
    ]
    keys_in = pltpu.make_async_copy(gid_far, gid, sems.at[1])
    table_in = pltpu.make_async_copy(table_far, table, sems.at[2])
    keys_in.start()
    table_in.start()
    for copy in values_in:
        copy.start()
    keys_in.wait()
    table_in.wait()
    slot = lookup(table[...], gid[...])
    slot_out[...] = slot
    sub = lax.broadcasted_iota(jnp.int32, (16, LANES), 0)
    ones = jnp.where(sub == 0, 1.0, 0.0).astype(BF16)
    spans = [slice(i * LANES, (i + 1) * LANES) for i in range(R // LANES)]
    high = jnp.where(slot >= HALF, 1.0, 0.0)
    highs = [jnp.broadcast_to(high[i : i + 1, :], (16, LANES)) for i in range(R // LANES)]
    picks = [((1.0 - h).astype(BF16), h.astype(BF16)) for h in highs]

    def place(rows, at, value, pick):
        split[rows : rows + 16, at] = value * pick[0]
        split[LHS + rows : LHS + rows + 16, at] = value * pick[1]

    for at, pick in zip(spans, picks):
        place(128, at, ones, pick)
    for g in range(4):
        values_in[g].wait()
        for at, pick in zip(spans, picks):
            a, b, _ = pieces(vt[16 * g : 16 * g + 16, at])
            place(16 * g, at, a, pick)
            place(64 + 16 * g, at, b, pick)
    for i, block in enumerate(columns(slot)):
        cols[i * LANES : (i + 1) * LANES, :] = block
    lane = lax.broadcasted_iota(jnp.int32, (T, T), 1)
    first = lax.broadcasted_iota(jnp.int32, (8, LANES), 0) == 0
    for j in range(NH):
        res = None
        for k in range(NT):
            at = slice(k * T, (k + 1) * T)
            keys = jnp.bitwise_and(cols[at, :], HALF - 1)
            keys = jnp.concatenate([keys, keys], axis=1)
            part = dot(split[:, at], hot(keys == lane + j * T))
            res = part if res is None else res + part
        for h in range(2):
            of = res[h * LHS : (h + 1) * LHS]
            total = of[0:64] + of[64:128]
            to = owner(h * NH + j)
            out[to, 0:64, :] = total[:, :LANES]
            out[to, 64:128, :] = total[:, LANES:]
            number = jnp.broadcast_to(of[128:129], (8, T))
            out[to, 128:136, :] = jnp.where(first, number[:, :LANES], number[:, LANES:])


def slice_kernel(arrived, out):
    total = arrived[0]
    for i in range(1, SIB):
        total = total + arrived[i]
    for p in range(RING):
        out[p, 0:16, :] = total[16 * p : 16 * p + 16]
        out[p, 16:24, :] = total[128:136]


def ring_kernel(arrived, out):
    total = arrived[0]
    for i in range(1, RING):
        total = total + arrived[i]
    for p in range(RING):
        out[p] = total


def scan_kernel(arrived, rings, out, counts_out):
    y = lax.axis_index("y")
    z = lax.axis_index("z")
    total = rings[0]
    before = jnp.where(y > 0, total, 0.0)
    for i in range(1, RING):
        ring = rings[i]
        before = before + jnp.where(i < y, ring, 0.0)
        total = total + ring
    number = jnp.where(z < RING // 2, total[16:17], total[17:18])
    closing = total[0:16] / jnp.maximum(number, 1.0)
    counts = before[16:24]
    acc = before[0:16]
    for p in range(RING):
        out[p, 0:16, :] = acc
        out[p, 16:32, :] = closing
        acc = acc + arrived[p, 0:16, :]
        counts = counts + jnp.where(p < z, arrived[p, 16:24, :], 0.0)
    counts_out[...] = counts


def start_kernel(far, arrived, counts, out_far, closing, out, sems):
    parts = []
    for p in range(RING):
        parts.append(far[p, 0:16, :])
        closing[16 * p : 16 * p + 16, :] = far[p, 16:32, :]
    acc = jnp.concatenate(parts + [counts[...]], axis=0)
    copies = []
    for k in range(SIB):
        out[k] = acc
        copies.append(pltpu.make_async_copy(out.at[k], out_far.at[k], sems.at[k]))
        copies[-1].start()
        acc = acc + arrived[k]
    for copy in copies:
        copy.wait()


def both(slot, j):
    return jnp.concatenate([slot[2 * j : 2 * j + 1, :], slot[2 * j + 1 : 2 * j + 2, :]], axis=1)


def own_kernel(split, slot, cols, out, local):
    local[...] = split[0:LHS, :] + split[LHS : 2 * LHS, :]
    label = lax.broadcasted_iota(jnp.int32, (T, T), 0)
    order = label <= lax.broadcasted_iota(jnp.int32, (T, T), 1)
    for j in range(NT):
        row = jnp.broadcast_to(both(slot, j), (T, T))
        own = None
        for k in range(j + 1):
            at = slice(k * T, (k + 1) * T)
            keys = cols[at, :]
            mask = jnp.concatenate([keys, keys], axis=1) == row
            if k == j:
                mask = jnp.logical_and(mask, order)
            part = dot(local[:, at], hot(mask))
            own = part if own is None else own + part
        at = slice(j * T, (j + 1) * T)
        out[0:64, at] = own[0:64] + own[64:128]
        out[64:72, at] = own[128:136]


def running_kernel(start, own, slot, closed, mean, count_far, closing_far, left, held_mean, count, closing, sems):
    for c in range(2):
        for h in range(2):
            closing[:, c * T + h * LANES : c * T + (h + 1) * LANES] = closed[c, h * 64 : (h + 1) * 64, :]
    copies = [pltpu.make_async_copy(closing, closing_far, sems.at[NT])]
    copies[0].start()
    sub = lax.broadcasted_iota(jnp.int32, (16, LANES), 0)
    for j in range(NT):
        for h in range(2):
            a, b, _ = pieces(start[owner(j), h * 64 : (h + 1) * 64, :])
            n = pieces(start[owner(j), 128 + h : 129 + h, :])
            n = [jnp.broadcast_to(v.astype(F32), (16, LANES)) for v in n]
            n = jnp.where(sub == 0, n[0], jnp.where(sub == 1, n[1], jnp.where(sub == 2, n[2], 0.0)))
            top = (j // NW) * LHS
            at = (j % NW) * T + h * LANES
            left[top : top + LHS, at : at + LANES] = jnp.concatenate([a, b, n.astype(BF16)], axis=0)
    label = lax.broadcasted_iota(jnp.int32, (T, T), 0)
    for j in range(NT):
        row = both(slot, j)
        high = jnp.broadcast_to(jnp.right_shift(row, 9), (LHS, T))
        low = jnp.bitwise_and(jnp.broadcast_to(row, (T, T)), PART - 1)
        res = None
        for k in range(NW):
            part = dot(left[:, k * T : (k + 1) * T], hot(label + k * T == low))
            res = part if res is None else res + part
        found = res[0:LHS]
        for w in range(1, WAYS):
            found = jnp.where(high == w, res[w * LHS : (w + 1) * LHS], found)
        res = found
        at = slice(j * T, (j + 1) * T)
        total = res[0:64] + res[64:128] + own[0:64, at]
        tally = (res[128:129] + res[129:130]) + res[130:131] + own[64:65, at]
        held_mean[:, at] = total / tally
        copies.append(pltpu.make_async_copy(held_mean.at[:, at], mean.at[:, at], sems.at[j]))
        copies[-1].start()
        whole = tally.astype(jnp.int32)
        count[2 * j : 2 * j + 1, :] = whole[:, :LANES]
        count[2 * j + 1 : 2 * j + 2, :] = whole[:, LANES:]
    copies.append(pltpu.make_async_copy(count, count_far, sems.at[NT + 1]))
    copies[-1].start()
    for copy in copies:
        copy.wait()


def shape(*dims, dtype=F32):
    return jax.ShapeDtypeStruct(dims, dtype)


def near(*dims, dtype=F32):
    return pltpu.VMEM(dims, dtype)


def outward(*dims):
    return pltpu.HBM(dims, F32)


def outer(x):
    return pltpu.with_memory_space_constraint(x, pltpu.HBM)


def held(x):
    return pltpu.with_memory_space_constraint(x, pltpu.VMEM)


def sums_call(vt, gid, table):
    outside = pl.BlockSpec(memory_space=pl.ANY)
    return pl.pallas_call(
        sums_kernel,
        in_specs=[outside] * 3,
        out_shape=(
            near(SIB, MSG, LANES),
            near(16, LANES, dtype=jnp.int32),
            near(2 * LHS, R, dtype=BF16),
            near(R, LANES, dtype=jnp.int32),
        ),
        scratch_shapes=[
            pltpu.VMEM((M, R), F32),
            pltpu.VMEM((16, LANES), jnp.int32),
            pltpu.VMEM((16, LANES), jnp.int32),
            pltpu.SemaphoreType.DMA((7,)),
        ],
        compiler_params=ROOM,
        name="local_sums",
    )(outer(vt), outer(gid), outer(table))


def own_call(split, slot, cols):
    return pl.pallas_call(
        own_kernel,
        out_shape=near(72, R),
        scratch_shapes=[pltpu.VMEM((LHS, R), BF16)],
        compiler_params=ROOM,
        cost_estimate=pl.CostEstimate(flops=2 * 144 * R * R // 2, bytes_accessed=1 << 20, transcendentals=0),
        name="own_rows",
    )(held(split), held(slot), held(cols))


def running_call(start, own, slot, closed):
    return pl.pallas_call(
        running_kernel,
        out_shape=(shape(M, R), shape(16, LANES, dtype=jnp.int32), shape(M, 512)),
        out_specs=(pl.BlockSpec(memory_space=pl.ANY),) * 3,
        scratch_shapes=[
            pltpu.VMEM((WAYS * LHS, PART), BF16),
            pltpu.VMEM((M, R), F32),
            pltpu.VMEM((16, LANES), jnp.int32),
            pltpu.VMEM((M, 2 * T), F32),
            pltpu.SemaphoreType.DMA((NT + 2,)),
        ],
        compiler_params=ROOM,
        name="running_means",
    )(start, held(own), held(slot), closed)


def local(values, group_ids, slot_of):
    vt = values.T
    gid = group_ids.reshape(16, LANES)
    table = slot_of.reshape(16, LANES)
    sums, slot, split, cols = sums_call(vt, gid, table)
    siblings = ("c", "x")
    arrived = held(lax.all_to_all(sums, siblings, 0, 0, tiled=True))
    parts = pl.pallas_call(
        slice_kernel,
        out_shape=near(RING, 24, LANES),
        compiler_params=ROOM,
        name="slice_sums",
    )(arrived)
    along_z = held(lax.all_to_all(parts, "z", 0, 0, tiled=True))
    ring = pl.pallas_call(
        ring_kernel,
        out_shape=near(RING, 24, LANES),
        compiler_params=ROOM,
        name="ring_sums",
    )(along_z)
    along_y = held(lax.all_to_all(ring, "y", 0, 0, tiled=True))
    scanned, counts = pl.pallas_call(
        scan_kernel,
        out_shape=(near(RING, 32, LANES), near(8, LANES)),
        compiler_params=ROOM,
        name="scan",
    )(along_z, along_y)
    back = held(lax.all_to_all(scanned, "z", 0, 0, tiled=True))
    starts, closing_half = pl.pallas_call(
        start_kernel,
        out_shape=(outward(SIB, MSG, LANES), near(LANES, LANES)),
        out_specs=(pl.BlockSpec(memory_space=pl.ANY), pl.BlockSpec(memory_space=pltpu.VMEM)),
        scratch_shapes=[pltpu.VMEM((SIB, MSG, LANES), F32), pltpu.SemaphoreType.DMA((SIB,))],
        compiler_params=ROOM,
        name="starts",
    )(back, arrived, counts)
    closed = held(lax.all_gather(closing_half, "c"))
    own = own_call(split, slot, cols)
    start = held(lax.all_to_all(starts, siblings, 0, 0, tiled=True))
    mean, count, closing = running_call(start, own, slot, closed)
    return mean.T, count.reshape(R), closing.T


def solution(mesh):
    split = Mesh(mesh.devices.reshape(8, 8, 2, 4), ROWS_ALL)
    in_specs = (P(ROWS_ALL, None), P(ROWS_ALL), P())
    out_specs = (P(ROWS_ALL, None), P(ROWS_ALL), P("x", None))
    return jax.shard_map(local, mesh=split, in_specs=in_specs, out_specs=out_specs, check_vma=False)
```

```python
import jax
import jax.numpy as jnp
from jax import lax
from jax.experimental import pallas as pl
from jax.experimental.pallas import tpu as pltpu
from jax.sharding import Mesh
from jax.sharding import PartitionSpec as P

ROWS_ALL = ("y", "z", "c", "x")
F32 = jnp.float32
BF16 = jnp.bfloat16
M = 64
R = 2048
S = 2048
LANES = 128
T = 256
NT = S // T
NH = NT // 2
WAYS = 4
PART = S // WAYS
NW = NT // WAYS
SIB = 8
FAR = 64
MSG = 136
LHS = 144
HALF = 1024


ROOM = pltpu.CompilerParams(vmem_limit_bytes=16 << 20)


def pieces(v):
    a = v.astype(BF16)
    rest = v - a.astype(F32)
    b = rest.astype(BF16)
    c = (rest - b.astype(F32)).astype(BF16)
    return a, b, c


def lookup(table, idx):
    low = jnp.bitwise_and(idx, LANES - 1)
    high = jnp.right_shift(idx, 7)
    out = jnp.zeros_like(idx)
    for k in range(S // LANES):
        row = jnp.broadcast_to(table[k : k + 1, :], idx.shape)
        out = jnp.where(high == k, jnp.take_along_axis(row, low, axis=1), out)
    return out


def columns(slot):
    flipped = jnp.concatenate([slot] * 8, axis=0).T
    return [jnp.broadcast_to(flipped[:, i : i + 1], (LANES, LANES)) for i in range(R // LANES)]


def dot(a, b):
    return lax.dot_general(a, b, (((1,), (0,)), ((), ())), preferred_element_type=F32)


def owner(block):
    return 4 * (block % 2) + block // 2


def hot(mask):
    return jnp.where(mask, 1.0, 0.0).astype(BF16)


def sums_kernel(vt_far, gid_far, table_far, out, slot_out, split, cols, vt, gid, table, sems):
    values_in = [
        pltpu.make_async_copy(vt_far.at[16 * g : 16 * g + 16], vt.at[16 * g : 16 * g + 16], sems.at[3 + g]) for g in range(4)
    ]
    keys_in = pltpu.make_async_copy(gid_far, gid, sems.at[1])
    table_in = pltpu.make_async_copy(table_far, table, sems.at[2])
    keys_in.start()
    table_in.start()
    for copy in values_in:
        copy.start()
    keys_in.wait()
    table_in.wait()
    slot = lookup(table[...], gid[...])
    slot_out[...] = slot
    sub = lax.broadcasted_iota(jnp.int32, (16, LANES), 0)
    ones = jnp.where(sub == 0, 1.0, 0.0).astype(BF16)
    spans = [slice(i * LANES, (i + 1) * LANES) for i in range(R // LANES)]
    high = jnp.where(slot >= HALF, 1.0, 0.0)
    highs = [jnp.broadcast_to(high[i : i + 1, :], (16, LANES)) for i in range(R // LANES)]
    picks = [((1.0 - h).astype(BF16), h.astype(BF16)) for h in highs]

    def place(rows, at, value, pick):
        split[rows : rows + 16, at] = value * pick[0]
        split[LHS + rows : LHS + rows + 16, at] = value * pick[1]

    for at, pick in zip(spans, picks):
        place(128, at, ones, pick)
    for g in range(4):
        values_in[g].wait()
        for at, pick in zip(spans, picks):
            a, b, _ = pieces(vt[16 * g : 16 * g + 16, at])
            place(16 * g, at, a, pick)
            place(64 + 16 * g, at, b, pick)
    for i, block in enumerate(columns(slot)):
        cols[i * LANES : (i + 1) * LANES, :] = block
    lane = lax.broadcasted_iota(jnp.int32, (T, T), 1)
    first = lax.broadcasted_iota(jnp.int32, (8, LANES), 0) == 0
    for j in range(NH):
        res = None
        for k in range(NT):
            at = slice(k * T, (k + 1) * T)
            keys = jnp.bitwise_and(cols[at, :], HALF - 1)
            keys = jnp.concatenate([keys, keys], axis=1)
            part = dot(split[:, at], hot(keys == lane + j * T))
            res = part if res is None else res + part
        for h in range(2):
            of = res[h * LHS : (h + 1) * LHS]
            total = of[0:64] + of[64:128]
            to = owner(h * NH + j)
            out[to, 0:64, :] = total[:, :LANES]
            out[to, 64:128, :] = total[:, LANES:]
            number = jnp.broadcast_to(of[128:129], (8, T))
            out[to, 128:136, :] = jnp.where(first, number[:, :LANES], number[:, LANES:])


def slice_kernel(arrived, out, buf):
    total = arrived[0]
    for i in range(1, SIB):
        total = total + arrived[i]
    buf[...] = total
    counts = buf[128:130, :]
    for p in range(FAR):
        out[p, 0:2, :] = buf[2 * p : 2 * p + 2, :]
        out[p, 2:4, :] = counts


def scan_kernel(arrived, out, counts_out):
    mine = lax.axis_index("y") * 8 + lax.axis_index("z")
    acc = jnp.zeros((4, LANES), F32)
    before = jnp.zeros((4, LANES), F32)
    for p in range(FAR):
        got = arrived[p]
        out[p, 0:2, :] = acc[0:2]
        before = before + jnp.where(p < mine, got, 0.0)
        acc = acc + got
    number = jnp.where(mine < FAR // 2, acc[2:3], acc[3:4])
    closing = acc[0:2] / jnp.maximum(number, 1.0)
    for p in range(FAR):
        out[p, 2:4, :] = closing
    counts_out[0:2, :] = before[2:4]


def start_kernel(far, arrived, counts, out_far, closing, out, buf, sems):
    for p in range(FAR):
        buf[2 * p : 2 * p + 2, :] = far[p, 0:2, :]
    buf[128:130, :] = counts[0:2, :]
    buf[130:136, :] = jnp.zeros((6, LANES), F32)
    acc = buf[...]
    copies = []
    for k in range(SIB):
        out[k] = acc
        copies.append(pltpu.make_async_copy(out.at[k], out_far.at[k], sems.at[k]))
        copies[-1].start()
        acc = acc + arrived[k]
    for p in range(FAR):
        closing[2 * p : 2 * p + 2, :] = far[p, 2:4, :]
    for copy in copies:
        copy.wait()


def both(slot, j):
    return jnp.concatenate([slot[2 * j : 2 * j + 1, :], slot[2 * j + 1 : 2 * j + 2, :]], axis=1)


def own_kernel(split, slot, cols, out, local):
    local[...] = split[0:LHS, :] + split[LHS : 2 * LHS, :]
    label = lax.broadcasted_iota(jnp.int32, (T, T), 0)
    order = label <= lax.broadcasted_iota(jnp.int32, (T, T), 1)
    for j in range(NT):
        row = jnp.broadcast_to(both(slot, j), (T, T))
        own = None
        for k in range(j + 1):
            at = slice(k * T, (k + 1) * T)
            keys = cols[at, :]
            mask = jnp.concatenate([keys, keys], axis=1) == row
            if k == j:
                mask = jnp.logical_and(mask, order)
            part = dot(local[:, at], hot(mask))
            own = part if own is None else own + part
        at = slice(j * T, (j + 1) * T)
        out[0:64, at] = own[0:64] + own[64:128]
        out[64:72, at] = own[128:136]


def running_kernel(start, own, slot, closed, mean, count_far, closing_far, left, held_mean, count, closing, sems):
    for c in range(2):
        for h in range(2):
            closing[:, c * T + h * LANES : c * T + (h + 1) * LANES] = closed[c, h * 64 : (h + 1) * 64, :]
    copies = [pltpu.make_async_copy(closing, closing_far, sems.at[NT])]
    copies[0].start()
    sub = lax.broadcasted_iota(jnp.int32, (16, LANES), 0)
    for j in range(NT):
        for h in range(2):
            a, b, _ = pieces(start[owner(j), h * 64 : (h + 1) * 64, :])
            n = pieces(start[owner(j), 128 + h : 129 + h, :])
            n = [jnp.broadcast_to(v.astype(F32), (16, LANES)) for v in n]
            n = jnp.where(sub == 0, n[0], jnp.where(sub == 1, n[1], jnp.where(sub == 2, n[2], 0.0)))
            top = (j // NW) * LHS
            at = (j % NW) * T + h * LANES
            left[top : top + LHS, at : at + LANES] = jnp.concatenate([a, b, n.astype(BF16)], axis=0)
    label = lax.broadcasted_iota(jnp.int32, (T, T), 0)
    for j in range(NT):
        row = both(slot, j)
        high = jnp.broadcast_to(jnp.right_shift(row, 9), (LHS, T))
        low = jnp.bitwise_and(jnp.broadcast_to(row, (T, T)), PART - 1)
        res = None
        for k in range(NW):
            part = dot(left[:, k * T : (k + 1) * T], hot(label + k * T == low))
            res = part if res is None else res + part
        found = res[0:LHS]
        for w in range(1, WAYS):
            found = jnp.where(high == w, res[w * LHS : (w + 1) * LHS], found)
        res = found
        at = slice(j * T, (j + 1) * T)
        total = res[0:64] + res[64:128] + own[0:64, at]
        tally = (res[128:129] + res[129:130]) + res[130:131] + own[64:65, at]
        held_mean[:, at] = total / tally
        copies.append(pltpu.make_async_copy(held_mean.at[:, at], mean.at[:, at], sems.at[j]))
        copies[-1].start()
        whole = tally.astype(jnp.int32)
        count[2 * j : 2 * j + 1, :] = whole[:, :LANES]
        count[2 * j + 1 : 2 * j + 2, :] = whole[:, LANES:]
    copies.append(pltpu.make_async_copy(count, count_far, sems.at[NT + 1]))
    copies[-1].start()
    for copy in copies:
        copy.wait()


def shape(*dims, dtype=F32):
    return jax.ShapeDtypeStruct(dims, dtype)


def near(*dims, dtype=F32):
    return pltpu.VMEM(dims, dtype)


def outward(*dims):
    return pltpu.HBM(dims, F32)


def outer(x):
    return pltpu.with_memory_space_constraint(x, pltpu.HBM)


def held(x):
    return pltpu.with_memory_space_constraint(x, pltpu.VMEM)


def sums_call(vt, gid, table):
    outside = pl.BlockSpec(memory_space=pl.ANY)
    return pl.pallas_call(
        sums_kernel,
        in_specs=[outside] * 3,
        out_shape=(
            near(SIB, MSG, LANES),
            near(16, LANES, dtype=jnp.int32),
            near(2 * LHS, R, dtype=BF16),
            near(R, LANES, dtype=jnp.int32),
        ),
        scratch_shapes=[
            pltpu.VMEM((M, R), F32),
            pltpu.VMEM((16, LANES), jnp.int32),
            pltpu.VMEM((16, LANES), jnp.int32),
            pltpu.SemaphoreType.DMA((7,)),
        ],
        compiler_params=ROOM,
        name="local_sums",
    )(outer(vt), outer(gid), outer(table))


def own_call(split, slot, cols):
    return pl.pallas_call(
        own_kernel,
        out_shape=near(72, R),
        scratch_shapes=[pltpu.VMEM((LHS, R), BF16)],
        compiler_params=ROOM,
        cost_estimate=pl.CostEstimate(flops=2 * 144 * R * R // 2, bytes_accessed=1 << 20, transcendentals=0),
        name="own_rows",
    )(held(split), held(slot), held(cols))


def running_call(start, own, slot, closed):
    return pl.pallas_call(
        running_kernel,
        out_shape=(shape(M, R), shape(16, LANES, dtype=jnp.int32), shape(M, 512)),
        out_specs=(pl.BlockSpec(memory_space=pl.ANY),) * 3,
        scratch_shapes=[
            pltpu.VMEM((WAYS * LHS, PART), BF16),
            pltpu.VMEM((M, R), F32),
            pltpu.VMEM((16, LANES), jnp.int32),
            pltpu.VMEM((M, 2 * T), F32),
            pltpu.SemaphoreType.DMA((NT + 2,)),
        ],
        compiler_params=ROOM,
        name="running_means",
    )(start, held(own), held(slot), closed)


def local(values, group_ids, slot_of):
    vt = values.T
    gid = group_ids.reshape(16, LANES)
    table = slot_of.reshape(16, LANES)
    sums, slot, split, cols = sums_call(vt, gid, table)
    siblings = ("c", "x")
    arrived = held(lax.all_to_all(sums, siblings, 0, 0, tiled=True))
    far = ("y", "z")
    pieces_out = pl.pallas_call(
        slice_kernel,
        out_shape=near(FAR, 4, LANES),
        scratch_shapes=[pltpu.VMEM((MSG, LANES), F32)],
        compiler_params=ROOM,
        name="slice_sums",
    )(arrived)
    met = held(lax.all_to_all(pieces_out, far, 0, 0, tiled=True))
    scanned, counts = pl.pallas_call(
        scan_kernel,
        out_shape=(near(FAR, 4, LANES), near(8, LANES)),
        compiler_params=ROOM,
        name="scan",
    )(met)
    back = held(lax.all_to_all(scanned, far, 0, 0, tiled=True))
    starts, closing_half = pl.pallas_call(
        start_kernel,
        out_shape=(outward(SIB, MSG, LANES), near(LANES, LANES)),
        out_specs=(pl.BlockSpec(memory_space=pl.ANY), pl.BlockSpec(memory_space=pltpu.VMEM)),
        scratch_shapes=[
            pltpu.VMEM((SIB, MSG, LANES), F32),
            pltpu.VMEM((MSG, LANES), F32),
            pltpu.SemaphoreType.DMA((SIB,)),
        ],
        compiler_params=ROOM,
        name="starts",
    )(back, arrived, counts)
    closed = held(lax.all_gather(closing_half, "c"))
    own = own_call(split, slot, cols)
    start = held(lax.all_to_all(starts, siblings, 0, 0, tiled=True))
    mean, count, closing = running_call(start, own, slot, closed)
    return mean.T, count.reshape(R), closing.T


def solution(mesh):
    split = Mesh(mesh.devices.reshape(8, 8, 2, 4), ROWS_ALL)
    in_specs = (P(ROWS_ALL, None), P(ROWS_ALL), P())
    out_specs = (P(ROWS_ALL, None), P(ROWS_ALL), P("x", None))
    return jax.shard_map(local, mesh=split, in_specs=in_specs, out_specs=out_specs, check_vma=False)
```
